512 devices in a mesh: job: 2 (over y), ta: 16 (over z), xyz: 8 (over x), src: 2 (over core).
Axes of the slice: x: 8, y: 2, z: 16, core: 2. Of those that a mesh axis runs over, the one named last changes fastest.
The devices are a block of a 8x16x16 slice.
Arguments:
- spinors: float32 [64, 32, 2, 8, 3, 2048], P('src', 'ta', None, 'job', None, 'xyz'), parts along dimension 3, may hold values from -6 to 6
- eigvecs: float32 [32, 256, 2, 3, 2048], P('ta', 'job', None, None, 'xyz'), parts along dimension 1, may hold values from -0.0546875 to 0.0546875
- group_of: int32 [32], replicated, may hold values from 0 to 15, as said below
- source_ids: int32 [64], P('src'), may hold values from 0 to 63, as said below
Outputs:
- perambulator: float32 [32, 2, 8, 64, 128], P('ta', None, 'job', 'src', 'xyz'), parts along dimension 2
The draws below stay inside these ranges and needn't reach their ends.
There are 2 independent parts, one for each index of `job`. The reference program is written for one: setup_inputs(seed, part) draws one part's arguments, and reference() takes and returns one part's arrays. A program takes and returns all parts, laid end to end along the dimension named above; an argument that names none is the same for every part. Nothing has to cross between parts.
Inputs may be any that keep to these rules, and one draw needn't show every extreme that they name: `group_of`: every group number appears exactly 2 times. `source_ids`: the 32 entries held by index i of src are a permutation of i * 32 to (i + 1) * 32 - 1.
All inputs are finite; a program needn't handle non-finite values.
Results may differ from the reference program's by a relative error of at most 0.00007.
Values sent between devices are 32-bit elements; how exact they have to be, the bound alone decides.
No kernel may reach another device: no remote copies, remote signals or barrier semaphores. Data moves between devices by JAX's collectives and lax.ppermute only.
A program may use at most 64 MiB of HBM per device.

```python
import jax
import jax.numpy as jnp
from jax import lax

K = 128
TL = 2
NS = 32
NT = 32
SITES = 2048
NSRC = 64


def draw_group_of(key, part):
    scores = jax.random.randint(key, (NT,), 0, 1 << 20) * NT + jnp.arange(NT, dtype=jnp.int32)
    shuffle = jnp.argsort(scores).astype(jnp.int32)
    return (jnp.argsort(shuffle).astype(jnp.int32) // TL).astype(jnp.int32)


def draw_source_ids(key, part):
    scores = jax.random.randint(key, (NSRC,), 0, 1 << 20) * NSRC + jnp.arange(NSRC, dtype=jnp.int32)
    blocks = scores.reshape(NSRC // NS, NS)
    within = jnp.argsort(blocks, axis=1).astype(jnp.int32)
    offsets = (jnp.arange(NSRC // NS, dtype=jnp.int32) * NS)[:, None]
    return (within + offsets).reshape(NSRC).astype(jnp.int32)


def levels(own_key, shape, pieces, least, top_value):
    def one(dim, blocks):
        steps = jax.random.uniform(jax.random.fold_in(jax.random.fold_in(own_key, 6), dim), (blocks,), jnp.float32, least / len(pieces), top_value / len(pieces))
        return jnp.repeat(jnp.exp(steps), shape[dim] // blocks).reshape((-1,) + (1,) * (len(shape) - dim - 1))

    loudness = one(*pieces[0])
    for cut in pieces[1:]:
        loudness = loudness * one(*cut)
    return loudness


def centred(rng, shape, width, most, cuts=(), kind=jnp.bfloat16):
    entries = width * jax.random.normal(rng, shape, jnp.float32)
    if cuts:
        entries = entries * levels(rng, shape, cuts, -0.22, 0.18)
    return jnp.clip(entries, -most, most).astype(kind)


def setup_inputs(seed: int = 0, part: int = 0) -> dict:
    streams_of = jax.random.split(jax.random.key(seed), 5)
    part_splits = jax.random.split(jax.random.fold_in(streams_of[4], part), 5)
    return {
        "spinors": centred(part_splits[0], (NSRC, NT, 2, 4, 3, SITES), 1.0, 6.0, ((0, 2), (1, 16), (5, 8)), jnp.float32),
        "eigvecs": centred(part_splits[1], (NT, K, 2, 3, SITES), (6 * SITES) ** -0.5, 0.0546875, ((0, 16), (4, 8)), jnp.float32),
        "group_of": draw_group_of(jax.random.fold_in(streams_of[4], 71), part),
        "source_ids": draw_source_ids(jax.random.fold_in(streams_of[4], 71), part),
    }


def contract_pair(vectors, spinor):
    vector_real = vectors[:, :, 0]
    vector_imag = vectors[:, :, 1]
    spinor_real = spinor[:, :, 0]
    spinor_imag = spinor[:, :, 1]

    def contract(left_side, right_side):
        return jnp.einsum("tkcx,ntscx->tsnk", left_side, right_side, precision=lax.Precision.HIGHEST)

    real_part = contract(vector_real, spinor_real) + contract(vector_imag, spinor_imag)
    imag_part = contract(vector_real, spinor_imag) - contract(vector_imag, spinor_real)
    return jnp.stack([real_part, imag_part], axis=1)


def reference(spinors, eigvecs, group_of, source_ids):
    extent = group_of.shape[0]
    sort_keys = group_of.astype(jnp.int32) * extent + jnp.arange(extent, dtype=jnp.int32)
    ordering = jnp.argsort(sort_keys).astype(jnp.int32)

    def one_slice(position):
        timeslice = ordering[position]
        vectors = lax.dynamic_slice_in_dim(eigvecs, position, 1, 0)
        spinor = lax.dynamic_slice_in_dim(spinors, timeslice, 1, 1)
        return contract_pair(vectors, spinor)[0]

    projected = lax.map(one_slice, jnp.arange(extent, dtype=jnp.int32))
    inverse = jnp.argsort(source_ids).astype(jnp.int32)
    return jnp.take(projected, inverse, axis=3)
```

```python
import jax
import jax.numpy as jnp
from jax import lax
from jax.sharding import PartitionSpec as P


def rank_of(keys):
    extent = keys.shape[0]
    index = jnp.arange(extent, dtype=jnp.int32)
    before = (keys[None, :] < keys[:, None]) | (
        (keys[None, :] == keys[:, None]) & (index[None, :] < index[:, None])
    )
    return jnp.sum(before.astype(jnp.int32), axis=1)


def inverse_of(rank):
    extent = rank.shape[0]
    index = jnp.arange(extent, dtype=jnp.int32)
    hit = rank[None, :] == index[:, None]
    return jnp.sum(jnp.where(hit, index[None, :], 0), axis=1)


def project(vectors, spinor):
    def contract(left, right):
        return jnp.einsum("bticx,ntscx->tsnbi", left, right, precision=lax.Precision.HIGHEST)

    vr, vi = vectors[:, :, :, 0], vectors[:, :, :, 1]
    pr, pi = spinor[:, :, 0], spinor[:, :, 1]
    real = contract(vr, pr) + contract(vi, pi)
    imag = contract(vr, pi) - contract(vi, pr)
    return jnp.stack([real, imag], axis=1)


def local(spinors, eigvecs, group_of, source_ids):
    nta, nx, nsrc = lax.axis_size("ta"), lax.axis_size("xyz"), lax.axis_size("src")
    core = lax.axis_index("src")
    ta = lax.axis_index("ta")
    rows, k = eigvecs.shape[0], eigvecs.shape[1]
    rest = eigvecs.shape[2:]
    n, tl = spinors.shape[0], spinors.shape[1]
    mine = k // nsrc
    part = mine // nta
    per_x = mine // nx

    rank = rank_of(group_of)
    ordering = inverse_of(rank)

    share = eigvecs.reshape(rows, nx, nsrc, per_x, *rest)
    share = lax.dynamic_index_in_dim(share, core, 2, keepdims=False)
    share = share.reshape(rows, nta, part, *rest)
    spread = lax.all_to_all(share, "ta", split_axis=1, concat_axis=0, tiled=False)
    spread = spread.reshape(nta * rows, part, *rest)
    picked = jnp.take(spread, rank, axis=0)
    sent = lax.all_to_all(picked.reshape(nta, tl, part, *rest), "ta", 0, 0, tiled=True)

    held = jnp.take(spinors, inverse_of(source_ids - n * core), axis=0)
    swap = [(i, nsrc - 1 - i) for i in range(nsrc)]
    other = lax.ppermute(held, "src", swap)

    mine_out = project(sent, held)
    other_out = project(sent, other)
    first = core == 0
    pair = jnp.stack(
        [jnp.where(first, mine_out, other_out), jnp.where(first, other_out, mine_out)], axis=0
    )
    s = spinors.shape[3]
    pair = pair.reshape(nsrc, tl, 2, s, n, nx, per_x)
    pair = jnp.moveaxis(pair, 5, 0).reshape(nx * nsrc, tl, 2, s, n, per_x)
    got = lax.all_to_all(pair, ("xyz", "src"), 0, 0, tiled=True)
    summed = jnp.sum(got.reshape(nx, nsrc, tl, 2, s, n, per_x), axis=0)
    summed = jnp.moveaxis(summed, 0, 4).reshape(tl, 2, s, n, nsrc * per_x)
    everyone = lax.all_gather(summed, "ta", axis=0, tiled=True)
    wanted = lax.dynamic_slice_in_dim(ordering, ta * tl, tl, 0)
    return jnp.take(everyone, wanted, axis=0)


def solution(mesh):
    in_specs = (
        P("src", "ta", None, "job", None, "xyz"),
        P("ta", "job", None, None, "xyz"),
        P(),
        P("src"),
    )
    out_specs = P("ta", None, "job", "src", "xyz")
    return jax.shard_map(local, mesh=mesh, in_specs=in_specs, out_specs=out_specs, check_vma=False)
```

```python
import functools

import jax
import jax.numpy as jnp
from jax import lax
from jax.experimental import pallas as pl
from jax.experimental.pallas import tpu as pltpu
from jax.sharding import PartitionSpec as P

LANES = 128


def rank_of(keys):
    extent = keys.shape[0]
    index = jnp.arange(extent, dtype=jnp.int32)
    before = (keys[None, :] < keys[:, None]) | (
        (keys[None, :] == keys[:, None]) & (index[None, :] < index[:, None])
    )
    return jnp.sum(before.astype(jnp.int32), axis=1)


def inverse_of(rank):
    extent = rank.shape[0]
    index = jnp.arange(extent, dtype=jnp.int32)
    hit = rank[None, :] == index[:, None]
    return jnp.sum(jnp.where(hit, index[None, :], 0), axis=1)


def pick_rows_kernel(index_ref, table_ref, out_ref, sem):
    count = out_ref.shape[0]
    copies = [
        pltpu.make_async_copy(table_ref.at[index_ref[i]], out_ref.at[i], sem.at[i])
        for i in range(count)
    ]
    for copy in copies:
        copy.start()
    for copy in copies:
        copy.wait()


def pick_rows(table, index):
    count = index.shape[0]
    return pl.pallas_call(
        pick_rows_kernel,
        out_shape=jax.ShapeDtypeStruct((count, *table.shape[1:]), table.dtype),
        in_specs=[
            pl.BlockSpec(memory_space=pltpu.SMEM),
            pl.BlockSpec(memory_space=pl.ANY),
        ],
        out_specs=pl.BlockSpec(memory_space=pl.ANY),
        scratch_shapes=[pltpu.SemaphoreType.DMA((count,))],
        name="pick_rows",
    )(index, table)


def halves(x):
    high = x.astype(jnp.bfloat16)
    low = (x - high.astype(jnp.float32)).astype(jnp.bfloat16)
    return high, low


def product_kernel(tl, parts, cols, core_ref, v_ref, hh, hl, oh, ol, out_ref, a_hi, a_lo, b_hi, b_lo):
    nz = v_ref.shape[0] // (tl * parts * cols * 2)
    stride = tl * parts * cols * 2
    half = parts * nz
    core = core_ref[0]

    def dot(left, right):
        return lax.dot_general(
            left, right, (((1,), (1,)), ((), ())), preferred_element_type=jnp.float32
        )

    for t in range(tl):
        for i in range(parts):
            for b in range(cols):
                start = ((t * parts + i) * cols + b) * 2
                real = v_ref[pl.ds(start, nz, stride=stride), :]
                imag = v_ref[pl.ds(start + 1, nz, stride=stride), :]
                real_hi, real_lo = halves(real)
                imag_hi, imag_lo = halves(imag)
                top = pl.ds(i * nz, nz)
                low = pl.ds(half + i * nz, nz)
                lane = pl.ds(b * LANES, LANES)
                a_hi[t, top, lane] = real_hi
                a_lo[t, top, lane] = real_lo
                a_hi[t, low, lane] = -imag_hi
                a_lo[t, low, lane] = -imag_lo
                b_hi[t, top, lane] = imag_hi
                b_lo[t, top, lane] = imag_lo
                b_hi[t, low, lane] = real_hi
                b_lo[t, low, lane] = real_lo
        ah, al, bh, bl = a_hi[t], a_lo[t], b_hi[t], b_lo[t]
        for slot, high, low in ((core, hh, hl), (1 - core, oh, ol)):
            total = dot(ah, high[t, 0]) + dot(bh, high[t, 1])
            total += dot(ah, low[t, 0]) + dot(bh, low[t, 1])
            total += dot(al, high[t, 0]) + dot(bl, high[t, 1])
            nx = out_ref.shape[0]
            per = half // nx
            for ri in range(2):
                for x in range(nx):
                    out_ref[x, slot, t, ri] = total[ri * half + x * per : ri * half + (x + 1) * per]


def final_kernel(order_ref, in_ref, out_ref):
    nsk, nri, nj = in_ref.shape[1], in_ref.shape[3], in_ref.shape[4]
    ns, n = out_ref.shape[2], out_ref.shape[4]
    for sk in range(nsk):
        for ri in range(nri):
            value = in_ref[0, sk, 0, ri]
            for s in range(ns):
                out_ref[0, ri, s, sk * nj : (sk + 1) * nj, :] = value[:, s * n : (s + 1) * n]


def local(spinors, eigvecs, group_of, source_ids):
    nta, nx, nsrc = lax.axis_size("ta"), lax.axis_size("xyz"), lax.axis_size("src")
    core = lax.axis_index("src").astype(jnp.int32)
    ta = lax.axis_index("ta").astype(jnp.int32)
    rows, k, _, nc, sites = eigvecs.shape
    n, tl, _, ns = spinors.shape[:4]
    mine = k // nsrc
    part = mine // nta
    per_x = mine // nx
    fold = nta // per_x
    blocks = sites // LANES
    cols = nc * blocks

    rank = rank_of(group_of)
    ordering = inverse_of(rank)

    share = eigvecs.reshape(rows, part, fold, nsrc, per_x, 2, nc, blocks, LANES)
    share = lax.dynamic_index_in_dim(share, core, 3, keepdims=False)
    share = share.transpose(2, 3, 0, 1, 5, 6, 4, 7)
    share = share.reshape(nta, rows * part * cols * 2, LANES)
    spread = lax.all_to_all(share, "ta", 0, 0, tiled=True)
    spread = spread.reshape(nta * rows, part * cols * 2, LANES)
    picked = pick_rows(spread, rank)
    picked = picked.reshape(nta, tl * part * cols * 2, LANES)
    sent = lax.all_to_all(picked, "ta", 0, 0, tiled=True)
    sent = sent.reshape(nta * tl * part * cols * 2, LANES)

    inverse = inverse_of(source_ids - n * core)
    held = spinors.at[inverse].get(mode="promise_in_bounds")
    held = held.transpose(1, 2, 3, 0, 4, 5).reshape(tl, 2, ns * n, nc * sites)
    other = lax.ppermute(held, "src", [(i, nsrc - 1 - i) for i in range(nsrc)])

    def split(x):
        high = lax.reduce_precision(x, 8, 7)
        return high.astype(jnp.bfloat16), (x - high).astype(jnp.bfloat16)

    held_hi, held_lo = split(held)
    other_hi, other_lo = split(other)

    wide = nc * sites
    pair = pl.pallas_call(
        functools.partial(product_kernel, tl, part, cols),
        out_shape=jax.ShapeDtypeStruct((nx, nsrc, tl, 2, per_x, ns * n), jnp.float32),
        in_specs=[pl.BlockSpec(memory_space=pltpu.SMEM)]
        + [pl.BlockSpec(memory_space=pltpu.VMEM)] * 5,
        out_specs=pl.BlockSpec(memory_space=pltpu.VMEM),
        scratch_shapes=[pltpu.VMEM((tl, 2 * mine, wide), jnp.bfloat16)] * 4,
        name="product",
    )(core[None], sent, held_hi, held_lo, other_hi, other_lo)

    pair = pair.reshape(nx * nsrc, tl * 2 * per_x, ns * n)
    got = lax.all_to_all(pair, ("xyz", "src"), 0, 0, tiled=True)
    summed = jnp.sum(got.reshape(nx, nsrc * tl * 2 * per_x, ns * n), axis=0)
    everyone = lax.all_gather(summed, "ta", axis=0, tiled=False)
    everyone = everyone.reshape(nta, nsrc, tl, 2, per_x, ns * n)
    wanted = lax.dynamic_slice_in_dim(ordering, ta * rows, rows, 0)
    out = pl.pallas_call(
        final_kernel,
        out_shape=jax.ShapeDtypeStruct((rows, 2, ns, nsrc * per_x, n), jnp.float32),
        grid_spec=pltpu.PrefetchScalarGridSpec(
            num_scalar_prefetch=1,
            grid=(rows,),
            in_specs=[
                pl.BlockSpec(
                    (1, nsrc, 1, 2, per_x, ns * n),
                    lambda r, order: (order[r] // tl, 0, order[r] % tl, 0, 0, 0),
                )
            ],
            out_specs=pl.BlockSpec((1, 2, ns, nsrc * per_x, n), lambda r, order: (r, 0, 0, 0, 0)),
        ),
        name="final",
    )(wanted, everyone)
    return out.transpose(0, 1, 2, 4, 3)


def solution(mesh):
    in_specs = (
        P("src", "ta", None, "job", None, "xyz"),
        P("ta", "job", None, None, "xyz"),
        P(),
        P("src"),
    )
    out_specs = P("ta", None, "job", "src", "xyz")
    return jax.shard_map(local, mesh=mesh, in_specs=in_specs, out_specs=out_specs, check_vma=False)
```

```python
import jax
import jax.numpy as jnp
from jax import lax
from jax.experimental import pallas as pl
from jax.experimental.pallas import tpu as pltpu
from jax.sharding import Mesh
from jax.sharding import PartitionSpec as P


def rank_of(keys):
    extent = keys.shape[0]
    index = jnp.arange(extent, dtype=jnp.int32)
    before = (keys[None, :] < keys[:, None]) | (
        (keys[None, :] == keys[:, None]) & (index[None, :] < index[:, None])
    )
    return jnp.sum(before.astype(jnp.int32), axis=1)


def inverse_of(rank):
    extent = rank.shape[0]
    index = jnp.arange(extent, dtype=jnp.int32)
    hit = rank[None, :] == index[:, None]
    return jnp.sum(jnp.where(hit, index[None, :], 0), axis=1)


def small(mib):
    return pltpu.CompilerParams(vmem_limit_bytes=mib << 20)


def share_kernel(core_ref, in_ref, out_ref, sem):
    rows, parts = in_ref.shape[:2]
    core = core_ref[0]
    copies = [
        pltpu.make_async_copy(
            in_ref.at[r, i, :, core], out_ref.at[:, :, r, i], sem.at[r * parts + i]
        )
        for r in range(rows)
        for i in range(parts)
    ]
    for copy in copies:
        copy.start()
    for copy in copies:
        copy.wait()


def pick_rows_kernel(index_ref, table_ref, out_ref, sem):
    count = out_ref.shape[0]
    copies = [
        pltpu.make_async_copy(table_ref.at[index_ref[i]], out_ref.at[i], sem.at[i])
        for i in range(count)
    ]
    for copy in copies:
        copy.start()
    for copy in copies:
        copy.wait()


def pick_rows(table, index):
    count = index.shape[0]
    return pl.pallas_call(
        pick_rows_kernel,
        out_shape=jax.ShapeDtypeStruct((count, *table.shape[1:]), table.dtype),
        in_specs=[
            pl.BlockSpec(memory_space=pltpu.SMEM),
            pl.BlockSpec(memory_space=pltpu.VMEM),
        ],
        out_specs=pl.BlockSpec(memory_space=pl.ANY),
        scratch_shapes=[pltpu.SemaphoreType.DMA((count,))],
        compiler_params=small(4),
        name="pick_rows",
    )(index, table)


def halves(x):
    high = x.astype(jnp.bfloat16)
    low = (x - high.astype(jnp.float32)).astype(jnp.bfloat16)
    return high, low


def product_kernel(core_ref, v_ref, hh, hl, oh, ol, out_ref, a_hi, a_lo, b_hi, b_lo):
    nz, tl, parts, nc, _, sites = v_ref.shape
    half = parts * nz
    nq, nx, _, _, piece, _ = out_ref.shape
    core = core_ref[0]

    def dot(left, right):
        return lax.dot_general(
            left, right, (((1,), (1,)), ((), ())), preferred_element_type=jnp.float32
        )

    for t in range(tl):
        for i in range(parts):
            for c in range(nc):
                real_hi, real_lo = halves(v_ref[:, t, i, c, 0, :])
                imag_hi, imag_lo = halves(v_ref[:, t, i, c, 1, :])
                top = pl.ds(i * nz, nz)
                low = pl.ds(half + i * nz, nz)
                lane = pl.ds(c * sites, sites)
                a_hi[t, top, lane] = real_hi
                a_lo[t, top, lane] = real_lo
                a_hi[t, low, lane] = -imag_hi
                a_lo[t, low, lane] = -imag_lo
                b_hi[t, top, lane] = imag_hi
                b_lo[t, top, lane] = imag_lo
                b_hi[t, low, lane] = real_hi
                b_lo[t, low, lane] = real_lo
        ah, al, bh, bl = a_hi[t], a_lo[t], b_hi[t], b_lo[t]
        for slot, high, low in ((core, hh, hl), (1 - core, oh, ol)):
            total = dot(ah, high[t, 0]) + dot(bh, high[t, 1])
            total += dot(ah, low[t, 0]) + dot(bh, low[t, 1])
            total += dot(al, high[t, 0]) + dot(bl, high[t, 1])
            per = half // nx
            for q in range(nq):
                ri, part = divmod(q, nq // 2)
                for x in range(nx):
                    first = ri * half + x * per + part * piece
                    out_ref[q, x, slot, t] = total[first : first + piece]


def sum_kernel(index_ref, in_ref, out_ref, held):
    near, nx, nsrc, tl = in_ref.shape[:4]
    for z in range(near):
        total = in_ref[z, 0]
        for x in range(1, nx):
            total += in_ref[z, x]
        for t in range(tl):
            for core in range(nsrc):
                held[z * tl + t, core] = total[core, t]
    for row in range(out_ref.shape[0]):
        out_ref[row] = held[index_ref[row]]


def final_kernel(order_ref, in_ref, out_ref):
    nq, nsrc, piece = in_ref.shape[1], in_ref.shape[3], in_ref.shape[4]
    ns, n = out_ref.shape[2], out_ref.shape[4]
    parts = nq // 2
    for core in range(nsrc):
        for ri in range(2):
            for part in range(parts):
                value = in_ref[0, ri * parts + part, 0, core]
                first = (core * parts + part) * piece
                for s in range(ns):
                    out_ref[0, ri, s, first : first + piece, :] = value[:, s * n : (s + 1) * n]


TA = ("tq", "tp")
NEAR = 4


def local(spinors, eigvecs, group_of, source_ids):
    nta, nx, nsrc = lax.axis_size(TA), lax.axis_size("xyz"), lax.axis_size("src")
    near = lax.axis_size("tp")
    core = lax.axis_index("src").astype(jnp.int32)
    ta = lax.axis_index(TA).astype(jnp.int32)
    rows, k, _, nc, sites = eigvecs.shape
    n, tl, _, ns = spinors.shape[:4]
    mine = k // nsrc
    part = mine // nta
    per_x = mine // nx
    fold = nta // per_x

    rank = rank_of(group_of)
    ordering = inverse_of(rank)

    tail = (nc, 2, sites)
    share = pl.pallas_call(
        share_kernel,
        out_shape=jax.ShapeDtypeStruct((fold, per_x, rows, part, *tail), jnp.float32),
        in_specs=[
            pl.BlockSpec(memory_space=pltpu.SMEM),
            pl.BlockSpec(memory_space=pl.ANY),
        ],
        out_specs=pl.BlockSpec(memory_space=pltpu.VMEM),
        scratch_shapes=[pltpu.SemaphoreType.DMA((rows * part,))],
        compiler_params=small(4),
        name="share",
    )(
        core[None],
        eigvecs.transpose(0, 1, 3, 2, 4).reshape(rows, part, fold, nsrc, per_x, *tail),
    )
    share = share.reshape(nta, rows, part, *tail)
    spread = lax.all_to_all(share, TA, 0, 0, tiled=True)
    picked = pick_rows(spread.reshape(nta * rows, part, *tail), rank)
    sent = lax.all_to_all(picked.reshape(nta, tl, part, *tail), TA, 0, 0, tiled=True)

    inverse = inverse_of(source_ids - n * core)
    held = spinors.at[inverse].get(mode="promise_in_bounds")
    held = held.transpose(1, 2, 3, 0, 4, 5).reshape(tl, 2, ns * n, nc * sites)
    other = lax.ppermute(held, "src", [(i, nsrc - 1 - i) for i in range(nsrc)])

    def split(x):
        high = lax.reduce_precision(x, 8, 7)
        return high.astype(jnp.bfloat16), (x - high).astype(jnp.bfloat16)

    held_hi, held_lo = split(held)
    other_hi, other_lo = split(other)

    piece = 2 * per_x // near
    pair = pl.pallas_call(
        product_kernel,
        out_shape=jax.ShapeDtypeStruct((near, nx, nsrc, tl, piece, ns * n), jnp.float32),
        in_specs=[pl.BlockSpec(memory_space=pltpu.SMEM)]
        + [pl.BlockSpec(memory_space=pltpu.VMEM)] * 5,
        out_specs=pl.BlockSpec(memory_space=pltpu.VMEM),
        scratch_shapes=[pltpu.VMEM((tl, 2 * mine, nc * sites), jnp.bfloat16)] * 4,
        compiler_params=small(16),
        name="product",
    )(core[None], sent, held_hi, held_lo, other_hi, other_lo)

    pair = pair.reshape(near * nx * nsrc, tl, piece, ns * n)
    got = lax.all_to_all(pair, ("tp", "xyz", "src"), 0, 0, tiled=True)
    here = jnp.clip(ordering - (ta // near) * (near * tl), 0, near * tl - 1)
    back = pl.pallas_call(
        sum_kernel,
        out_shape=jax.ShapeDtypeStruct((nta * rows, nsrc, piece, ns * n), jnp.float32),
        in_specs=[
            pl.BlockSpec(memory_space=pltpu.SMEM),
            pl.BlockSpec(memory_space=pltpu.VMEM),
        ],
        out_specs=pl.BlockSpec(memory_space=pltpu.VMEM),
        scratch_shapes=[pltpu.VMEM((near * tl, nsrc, piece, ns * n), jnp.float32)],
        compiler_params=small(4),
        name="sum_over_xyz",
    )(here, got.reshape(near, nx, nsrc, tl, piece, ns * n))

    home = lax.all_to_all(back.reshape(nta, rows, nsrc, piece, ns * n), TA, 0, 0, tiled=True)
    home = home.reshape(nta // near, near, rows, nsrc, piece, ns * n)
    wanted = lax.dynamic_slice_in_dim(ordering, ta * rows, rows, 0)
    out = pl.pallas_call(
        final_kernel,
        out_shape=jax.ShapeDtypeStruct((rows, 2, ns, nsrc * per_x, n), jnp.float32),
        grid_spec=pltpu.PrefetchScalarGridSpec(
            num_scalar_prefetch=1,
            grid=(rows,),
            in_specs=[
                pl.BlockSpec(
                    (1, near, 1, nsrc, piece, ns * n),
                    lambda r, order: (order[r] // (near * tl), 0, r, 0, 0, 0),
                )
            ],
            out_specs=pl.BlockSpec((1, 2, ns, nsrc * per_x, n), lambda r, order: (r, 0, 0, 0, 0)),
        ),
        compiler_params=small(4),
        name="final",
    )(wanted, home)
    return out.transpose(0, 1, 2, 4, 3)


def solution(mesh):
    shape = dict(mesh.shape)
    cut = (shape["job"], shape["ta"] // NEAR, NEAR, shape["xyz"], shape["src"])
    mesh = Mesh(mesh.devices.reshape(cut), ("job", *TA, "xyz", "src"))
    in_specs = (
        P("src", TA, None, "job", None, "xyz"),
        P(TA, "job", None, None, "xyz"),
        P(),
        P("src"),
    )
    out_specs = P(TA, None, "job", "src", "xyz")
    return jax.shard_map(local, mesh=mesh, in_specs=in_specs, out_specs=out_specs, check_vma=False)
```

```python
import functools

import jax
import jax.numpy as jnp
from jax import lax
from jax.experimental import pallas as pl
from jax.experimental.pallas import tpu as pltpu
from jax.sharding import Mesh
from jax.sharding import PartitionSpec as P


LANES = 128


def rank_of(keys):
    extent = keys.shape[0]
    index = jnp.arange(extent, dtype=jnp.int32)
    before = (keys[None, :] < keys[:, None]) | (
        (keys[None, :] == keys[:, None]) & (index[None, :] < index[:, None])
    )
    return jnp.sum(before.astype(jnp.int32), axis=1)


def inverse_of(rank):
    extent = rank.shape[0]
    index = jnp.arange(extent, dtype=jnp.int32)
    hit = rank[None, :] == index[:, None]
    return jnp.sum(jnp.where(hit, index[None, :], 0), axis=1)


def small(mib):
    return pltpu.CompilerParams(vmem_limit_bytes=mib << 20)


def share_kernel(core_ref, in_ref, out_ref, held, sem):
    rows, parts, folds, _, per_x, nc, _, sites = in_ref.shape
    core = core_ref[0]
    copies = [
        pltpu.make_async_copy(
            in_ref.at[r, i, :, core], held.at[r * parts + i], sem.at[r * parts + i]
        )
        for r in range(rows)
        for i in range(parts)
    ]
    for copy in copies:
        copy.start()
    for p, copy in enumerate(copies):
        copy.wait()
        line = p * nc * 2 * (sites // LANES)
        for c in range(nc):
            for lane in range(0, sites, LANES):
                for f in range(folds):
                    value = held[p, f, :, c, :, lane : lane + LANES]
                    out_ref[f * per_x : (f + 1) * per_x, line : line + 2, :] = value
                line += 2


def pick_rows_kernel(index_ref, table_ref, out_ref, sem):
    count = out_ref.shape[0]
    copies = [
        pltpu.make_async_copy(table_ref.at[index_ref[i]], out_ref.at[i], sem.at[i])
        for i in range(count)
    ]
    for copy in copies:
        copy.start()
    for copy in copies:
        copy.wait()


def pick_rows(table, index):
    count = index.shape[0]
    return pl.pallas_call(
        pick_rows_kernel,
        out_shape=jax.ShapeDtypeStruct((count, *table.shape[1:]), table.dtype),
        in_specs=[
            pl.BlockSpec(memory_space=pltpu.SMEM),
            pl.BlockSpec(memory_space=pltpu.VMEM),
        ],
        out_specs=pl.BlockSpec(memory_space=pl.ANY),
        scratch_shapes=[pltpu.SemaphoreType.DMA((count,))],
        compiler_params=small(4),
        name="pick_rows",
    )(index, table)


def halves(x):
    high = x.astype(jnp.bfloat16)
    low = (x - high.astype(jnp.float32)).astype(jnp.bfloat16)
    return high, low


def product_kernel(parts, core_ref, v_ref, hh, hl, oh, ol, out_ref, p_hi, p_lo, a_ref, b_ref, sem):
    nq, nx, nsrc, tl, piece, width = out_ref.shape
    wide = p_hi.shape[3]
    cols = wide // LANES
    half = a_ref.shape[1] // 4
    nz = half // parts
    core = core_ref[0]

    copies = []
    for t in range(tl):
        group = []
        for i, (own, src, dst) in enumerate(
            ((True, hh, p_hi), (False, oh, p_hi), (True, hl, p_lo), (False, ol, p_lo))
        ):
            first = (core if own else nsrc - 1 - core) * width
            group.append(
                pltpu.make_async_copy(
                    src.at[t], dst.at[t, :, pl.ds(pl.multiple_of(first, width), width)], sem.at[t, i]
                )
            )
            group[-1].start()
        copies.append(group)

    def dot(left, right):
        return lax.dot_general(
            left, right, (((1,), (1,)), ((), ())), preferred_element_type=jnp.float32
        )

    stride = tl * parts * cols * 2
    for t in range(tl):
        for i in range(parts):
            for b in range(cols):
                start = ((t * parts + i) * cols + b) * 2
                real_hi, real_lo = halves(v_ref[pl.ds(start, nz, stride=stride), :])
                imag_hi, imag_lo = halves(v_ref[pl.ds(start + 1, nz, stride=stride), :])
                lane = pl.ds(b * LANES, LANES)
                for j, (real, imag) in enumerate(((real_hi, imag_hi), (real_lo, imag_lo))):
                    top = pl.ds(2 * j * half + i * nz, nz)
                    low = pl.ds((2 * j + 1) * half + i * nz, nz)
                    a_ref[t, top, lane] = real
                    a_ref[t, low, lane] = -imag
                    b_ref[t, top, lane] = imag
                    b_ref[t, low, lane] = real
    per = half // nx
    for t in range(tl):
        for copy in copies[t]:
            copy.wait()
        both = dot(a_ref[t], p_hi[t, 0]) + dot(b_ref[t], p_hi[t, 1])
        total = both[: 2 * half] + both[2 * half :]
        total += dot(a_ref[t, : 2 * half], p_lo[t, 0]) + dot(b_ref[t, : 2 * half], p_lo[t, 1])
        for q in range(nq):
            ri, part = divmod(q, nq // 2)
            for x in range(nx):
                first = ri * half + x * per + part * piece
                for slot in range(nsrc):
                    out_ref[q, x, slot, t] = total[
                        first : first + piece, slot * width : (slot + 1) * width
                    ]


def sum_kernel(index_ref, in_ref, out_ref, held):
    near, nx, nsrc, tl = in_ref.shape[:4]
    for z in range(near):
        total = in_ref[z, 0]
        for x in range(1, nx):
            total += in_ref[z, x]
        for t in range(tl):
            for core in range(nsrc):
                held[z * tl + t, core] = total[core, t]
    for row in range(out_ref.shape[0]):
        out_ref[row] = held[index_ref[row]]


def final_kernel(order_ref, in_ref, out_ref):
    nq, nsrc, piece = in_ref.shape[1], in_ref.shape[3], in_ref.shape[4]
    ns, n = out_ref.shape[2], out_ref.shape[4]
    parts = nq // 2
    for core in range(nsrc):
        for ri in range(2):
            for part in range(parts):
                value = in_ref[0, ri * parts + part, 0, core]
                first = (core * parts + part) * piece
                for s in range(ns):
                    out_ref[0, ri, s, first : first + piece, :] = value[:, s * n : (s + 1) * n]


TA = ("tq", "tp")
NEAR = 4


def local(spinors, eigvecs, group_of, source_ids):
    nta, nx, nsrc = lax.axis_size(TA), lax.axis_size("xyz"), lax.axis_size("src")
    near = lax.axis_size("tp")
    core = lax.axis_index("src").astype(jnp.int32)
    ta = lax.axis_index(TA).astype(jnp.int32)
    rows, k, _, nc, sites = eigvecs.shape
    n, tl, _, ns = spinors.shape[:4]
    mine = k // nsrc
    part = mine // nta
    per_x = mine // nx
    fold = nta // per_x

    rank = rank_of(group_of)
    ordering = inverse_of(rank)

    tail = (nc, 2, sites)
    lines = part * nc * 2 * sites // LANES
    share = pl.pallas_call(
        share_kernel,
        out_shape=jax.ShapeDtypeStruct((nta, lines * rows, LANES), jnp.float32),
        in_specs=[
            pl.BlockSpec(memory_space=pltpu.SMEM),
            pl.BlockSpec(memory_space=pltpu.HBM),
        ],
        out_specs=pl.BlockSpec(memory_space=pltpu.VMEM),
        scratch_shapes=[
            pltpu.VMEM((rows * part, fold, per_x, *tail), jnp.float32),
            pltpu.SemaphoreType.DMA((rows * part,)),
        ],
        name="share",
    )(
        core[None],
        eigvecs.transpose(0, 1, 3, 2, 4).reshape(rows, part, fold, nsrc, per_x, *tail),
    )
    spread = lax.all_to_all(share, TA, 0, 0, tiled=True)
    picked = pick_rows(spread.reshape(nta * rows, lines, LANES), rank)
    sent = lax.all_to_all(picked.reshape(nta, tl * lines, LANES), TA, 0, 0, tiled=True)
    sent = sent.reshape(nta * tl * lines, LANES)

    inverse = inverse_of(source_ids - n * core)
    held = spinors.at[inverse].get(mode="promise_in_bounds")
    held = held.transpose(1, 2, 3, 0, 4, 5).reshape(tl, 2, ns * n, nc * sites)
    other = lax.ppermute(held, "src", [(i, nsrc - 1 - i) for i in range(nsrc)])

    def split(x):
        high = lax.reduce_precision(x, 8, 7)
        return high.astype(jnp.bfloat16), (x - high).astype(jnp.bfloat16)

    held_hi, held_lo = split(held)
    other_hi, other_lo = split(other)

    piece = 2 * per_x // near
    pair = pl.pallas_call(
        functools.partial(product_kernel, part),
        out_shape=jax.ShapeDtypeStruct((near, nx, nsrc, tl, piece, ns * n), jnp.float32),
        in_specs=[
            pl.BlockSpec(memory_space=pltpu.SMEM),
            pl.BlockSpec(memory_space=pltpu.VMEM),
        ]
        + [pl.BlockSpec(memory_space=pltpu.HBM)] * 4,
        out_specs=pl.BlockSpec(memory_space=pltpu.VMEM),
        scratch_shapes=[pltpu.VMEM((tl, 2, nsrc * ns * n, nc * sites), jnp.bfloat16)] * 2
        + [pltpu.VMEM((tl, 4 * mine, nc * sites), jnp.bfloat16)] * 2
        + [pltpu.SemaphoreType.DMA((tl, 4))],
        name="product",
    )(core[None], sent, held_hi, held_lo, other_hi, other_lo)

    pair = pair.reshape(near * nx * nsrc, tl, piece, ns * n)
    got = lax.all_to_all(pair, ("tp", "xyz", "src"), 0, 0, tiled=True)
    here = jnp.clip(ordering - (ta // near) * (near * tl), 0, near * tl - 1)
    back = pl.pallas_call(
        sum_kernel,
        out_shape=jax.ShapeDtypeStruct((nta * rows, nsrc, piece, ns * n), jnp.float32),
        in_specs=[
            pl.BlockSpec(memory_space=pltpu.SMEM),
            pl.BlockSpec(memory_space=pltpu.VMEM),
        ],
        out_specs=pl.BlockSpec(memory_space=pltpu.VMEM),
        scratch_shapes=[pltpu.VMEM((near * tl, nsrc, piece, ns * n), jnp.float32)],
        compiler_params=small(4),
        name="sum_over_xyz",
    )(here, got.reshape(near, nx, nsrc, tl, piece, ns * n))

    home = lax.all_to_all(back.reshape(nta, rows, nsrc, piece, ns * n), TA, 0, 0, tiled=True)
    home = home.reshape(nta // near, near, rows, nsrc, piece, ns * n)
    wanted = lax.dynamic_slice_in_dim(ordering, ta * rows, rows, 0)
    out = pl.pallas_call(
        final_kernel,
        out_shape=jax.ShapeDtypeStruct((rows, 2, ns, nsrc * per_x, n), jnp.float32),
        grid_spec=pltpu.PrefetchScalarGridSpec(
            num_scalar_prefetch=1,
            grid=(rows,),
            in_specs=[
                pl.BlockSpec(
                    (1, near, 1, nsrc, piece, ns * n),
                    lambda r, order: (order[r] // (near * tl), 0, r, 0, 0, 0),
                )
            ],
            out_specs=pl.BlockSpec((1, 2, ns, nsrc * per_x, n), lambda r, order: (r, 0, 0, 0, 0)),
        ),
        compiler_params=small(4),
        name="final",
    )(wanted, home)
    return out.transpose(0, 1, 2, 4, 3)


def solution(mesh):
    shape = dict(mesh.shape)
    cut = (shape["job"], shape["ta"] // NEAR, NEAR, shape["xyz"], shape["src"])
    mesh = Mesh(mesh.devices.reshape(cut), ("job", *TA, "xyz", "src"))
    in_specs = (
        P("src", TA, None, "job", None, "xyz"),
        P(TA, "job", None, None, "xyz"),
        P(),
        P("src"),
    )
    out_specs = P(TA, None, "job", "src", "xyz")
    return jax.shard_map(local, mesh=mesh, in_specs=in_specs, out_specs=out_specs, check_vma=False)
```

```python
import functools

import jax
import jax.numpy as jnp
from jax import lax
from jax.experimental import pallas as pl
from jax.experimental.pallas import tpu as pltpu
from jax.sharding import Mesh
from jax.sharding import PartitionSpec as P


LANES = 128


def rank_of(keys):
    extent = keys.shape[0]
    index = jnp.arange(extent, dtype=jnp.int32)
    before = (keys[None, :] < keys[:, None]) | (
        (keys[None, :] == keys[:, None]) & (index[None, :] < index[:, None])
    )
    return jnp.sum(before.astype(jnp.int32), axis=1)


def inverse_of(rank):
    extent = rank.shape[0]
    index = jnp.arange(extent, dtype=jnp.int32)
    hit = rank[None, :] == index[:, None]
    return jnp.sum(jnp.where(hit, index[None, :], 0), axis=1)


def small(mib):
    return pltpu.CompilerParams(vmem_limit_bytes=mib << 20)


def share_kernel(core_ref, in_ref, out_ref, held, packed, sem, out_sem):
    rows, parts, folds, _, per_x, nc, _, sites = in_ref.shape
    core = core_ref[0]
    copies = [
        pltpu.make_async_copy(
            in_ref.at[r, i, :, core], held.at[r * parts + i], sem.at[r * parts + i]
        )
        for r in range(rows)
        for i in range(parts)
    ]
    for copy in copies:
        copy.start()
    lines = out_ref.shape[1] // rows
    sends = []
    for r in range(rows):
        line = r * lines
        for i in range(parts):
            p = r * parts + i
            copies[p].wait()
            for c in range(nc):
                for lane in range(0, sites, LANES):
                    for f in range(folds):
                        value = held[p, f, :, c, :, lane : lane + LANES]
                        packed[f * per_x : (f + 1) * per_x, line : line + 2, :] = value
                    line += 2
        span = pl.ds(r * lines, lines)
        sends.append(
            pltpu.make_async_copy(packed.at[:, span], out_ref.at[:, span], out_sem.at[r])
        )
        sends[-1].start()
    for send in sends:
        send.wait()


def pick_rows_kernel(index_ref, table_ref, out_ref, sem):
    count = out_ref.shape[0]
    copies = [
        pltpu.make_async_copy(table_ref.at[index_ref[i]], out_ref.at[i], sem.at[i])
        for i in range(count)
    ]
    for copy in copies:
        copy.start()
    for copy in copies:
        copy.wait()


def pick_rows(table, index):
    count = index.shape[0]
    return pl.pallas_call(
        pick_rows_kernel,
        out_shape=jax.ShapeDtypeStruct((count, *table.shape[1:]), table.dtype),
        in_specs=[
            pl.BlockSpec(memory_space=pltpu.SMEM),
            pl.BlockSpec(memory_space=pltpu.VMEM),
        ],
        out_specs=pl.BlockSpec(memory_space=pl.ANY),
        scratch_shapes=[pltpu.SemaphoreType.DMA((count,))],
        compiler_params=small(4),
        name="pick_rows",
    )(index, table)


def halves(x):
    high = x.astype(jnp.bfloat16)
    low = (x - high.astype(jnp.float32)).astype(jnp.bfloat16)
    return high, low


def product_kernel(
    parts, core_ref, v_in, hh, hl, oh, ol, out_ref, v_ref, p_hi, p_lo, a_ref, b_ref, sem, v_sem
):
    nq, nx, nsrc, tl, piece, width = out_ref.shape
    wide = p_hi.shape[3]
    cols = wide // LANES
    half = a_ref.shape[1] // 4
    nz = half // parts
    core = core_ref[0]

    v_copy = pltpu.make_async_copy(v_in, v_ref, v_sem)
    v_copy.start()
    copies = []
    for t in range(tl):
        group = []
        for i, (own, src, dst) in enumerate(
            ((True, hh, p_hi), (False, oh, p_hi), (True, hl, p_lo), (False, ol, p_lo))
        ):
            first = (core if own else nsrc - 1 - core) * width
            group.append(
                pltpu.make_async_copy(
                    src.at[t], dst.at[t, :, pl.ds(pl.multiple_of(first, width), width)], sem.at[t, i]
                )
            )
            group[-1].start()
        copies.append(group)

    def dot(left, right):
        return lax.dot_general(
            left, right, (((1,), (1,)), ((), ())), preferred_element_type=jnp.float32
        )

    stride = tl * parts * cols * 2
    v_copy.wait()
    for t in range(tl):
        for i in range(parts):
            for b in range(cols):
                start = ((t * parts + i) * cols + b) * 2
                real_hi, real_lo = halves(v_ref[pl.ds(start, nz, stride=stride), :])
                imag_hi, imag_lo = halves(v_ref[pl.ds(start + 1, nz, stride=stride), :])
                lane = pl.ds(b * LANES, LANES)
                for j, (real, imag) in enumerate(((real_hi, imag_hi), (real_lo, imag_lo))):
                    top = pl.ds(2 * j * half + i * nz, nz)
                    low = pl.ds((2 * j + 1) * half + i * nz, nz)
                    a_ref[t, top, lane] = real
                    a_ref[t, low, lane] = -imag
                    b_ref[t, top, lane] = imag
                    b_ref[t, low, lane] = real
    per = half // nx
    for t in range(tl):
        for copy in copies[t]:
            copy.wait()
        both = dot(a_ref[t], p_hi[t, 0]) + dot(b_ref[t], p_hi[t, 1])
        total = both[: 2 * half] + both[2 * half :]
        total += dot(a_ref[t, : 2 * half], p_lo[t, 0]) + dot(b_ref[t, : 2 * half], p_lo[t, 1])
        for q in range(nq):
            ri, part = divmod(q, nq // 2)
            for x in range(nx):
                first = ri * half + x * per + part * piece
                for slot in range(nsrc):
                    out_ref[q, x, slot, t] = total[
                        first : first + piece, slot * width : (slot + 1) * width
                    ]


def sum_kernel(index_ref, in_ref, out_ref, held):
    near, nx, nsrc, tl = in_ref.shape[:4]
    nta, _, rows = out_ref.shape[:3]
    for z in range(near):
        total = in_ref[z, 0]
        for x in range(1, nx):
            total += in_ref[z, x]
        for t in range(tl):
            for core in range(nsrc):
                held[z * tl + t, core] = total[core, t]
    for ta in range(nta):
        for row in range(rows):
            value = held[index_ref[ta * rows + row]]
            for core in range(nsrc):
                out_ref[ta, core, row] = value[core]


def final_kernel(per_group, order_ref, in_ref, out_ref):
    _, nq, nsrc, rows, piece, _ = in_ref.shape
    ns, n = out_ref.shape[2], out_ref.shape[4]
    parts = nq // 2
    for row in range(rows):
        group = order_ref[row] // per_group
        for core in range(nsrc):
            for ri in range(2):
                for part in range(parts):
                    value = in_ref[group, ri * parts + part, core, row]
                    first = (core * parts + part) * piece
                    for s in range(ns):
                        out_ref[row, ri, s, first : first + piece, :] = value[
                            :, s * n : (s + 1) * n
                        ]


TA = ("tq", "tp")
NEAR = 4


def local(spinors, eigvecs, group_of, source_ids):
    nta, nx, nsrc = lax.axis_size(TA), lax.axis_size("xyz"), lax.axis_size("src")
    near = lax.axis_size("tp")
    core = lax.axis_index("src").astype(jnp.int32)
    ta = lax.axis_index(TA).astype(jnp.int32)
    rows, k, _, nc, sites = eigvecs.shape
    n, tl, _, ns = spinors.shape[:4]
    mine = k // nsrc
    part = mine // nta
    per_x = mine // nx
    fold = nta // per_x

    rank = rank_of(group_of)
    ordering = inverse_of(rank)

    tail = (nc, 2, sites)
    lines = part * nc * 2 * sites // LANES
    share = pl.pallas_call(
        share_kernel,
        out_shape=jax.ShapeDtypeStruct((nta, lines * rows, LANES), jnp.float32),
        in_specs=[
            pl.BlockSpec(memory_space=pltpu.SMEM),
            pl.BlockSpec(memory_space=pltpu.HBM),
        ],
        out_specs=pl.BlockSpec(memory_space=pltpu.HBM),
        scratch_shapes=[
            pltpu.VMEM((rows * part, fold, per_x, *tail), jnp.float32),
            pltpu.VMEM((nta, lines * rows, LANES), jnp.float32),
            pltpu.SemaphoreType.DMA((rows * part,)),
            pltpu.SemaphoreType.DMA((rows,)),
        ],
        name="share",
    )(
        core[None],
        eigvecs.transpose(0, 1, 3, 2, 4).reshape(rows, part, fold, nsrc, per_x, *tail),
    )
    spread = lax.all_to_all(share, TA, 0, 0, tiled=True)
    picked = pick_rows(spread.reshape(nta * rows, lines, LANES), rank)
    sent = lax.all_to_all(picked.reshape(nta, tl * lines, LANES), TA, 0, 0, tiled=True)
    sent = sent.reshape(nta * tl * lines, LANES)

    inverse = inverse_of(source_ids - n * core)
    held = spinors.at[inverse].get(mode="promise_in_bounds")
    held = held.transpose(1, 2, 3, 0, 4, 5).reshape(tl, 2, ns * n, nc * sites)
    other = lax.ppermute(held, "src", [(i, nsrc - 1 - i) for i in range(nsrc)])

    def split(x):
        high = lax.reduce_precision(x, 8, 7)
        return high.astype(jnp.bfloat16), (x - high).astype(jnp.bfloat16)

    held_hi, held_lo = split(held)
    other_hi, other_lo = split(other)

    piece = 2 * per_x // near
    pair = pl.pallas_call(
        functools.partial(product_kernel, part),
        out_shape=jax.ShapeDtypeStruct((near, nx, nsrc, tl, piece, ns * n), jnp.float32),
        in_specs=[pl.BlockSpec(memory_space=pltpu.SMEM)]
        + [pl.BlockSpec(memory_space=pltpu.HBM)] * 5,
        out_specs=pl.BlockSpec(memory_space=pltpu.VMEM),
        scratch_shapes=[pltpu.VMEM(sent.shape, jnp.float32)]
        + [pltpu.VMEM((tl, 2, nsrc * ns * n, nc * sites), jnp.bfloat16)] * 2
        + [pltpu.VMEM((tl, 4 * mine, nc * sites), jnp.bfloat16)] * 2
        + [pltpu.SemaphoreType.DMA((tl, 4)), pltpu.SemaphoreType.DMA],
        name="product",
    )(core[None], sent, held_hi, held_lo, other_hi, other_lo)

    pair = pair.reshape(near * nx, nsrc, tl, piece, ns * n)
    got = lax.all_to_all(pair, ("tp", "xyz"), 0, 0, tiled=True)
    here = jnp.clip(ordering - (ta // near) * (near * tl), 0, near * tl - 1)
    back = pl.pallas_call(
        sum_kernel,
        out_shape=jax.ShapeDtypeStruct((nta, nsrc, rows, piece, ns * n), jnp.float32),
        in_specs=[
            pl.BlockSpec(memory_space=pltpu.SMEM),
            pl.BlockSpec(memory_space=pltpu.VMEM),
        ],
        out_specs=pl.BlockSpec(memory_space=pltpu.VMEM),
        scratch_shapes=[pltpu.VMEM((near * tl, nsrc, piece, ns * n), jnp.float32)],
        compiler_params=small(4),
        name="sum_over_xyz",
    )(here, got.reshape(near, nx, nsrc, tl, piece, ns * n))

    back = back.reshape(nta * nsrc, rows, piece, ns * n)
    home = lax.all_to_all(back, (*TA, "src"), 0, 0, tiled=True)
    home = home.reshape(nta // near, near, nsrc, rows, piece, ns * n)
    wanted = lax.dynamic_slice_in_dim(ordering, ta * rows, rows, 0)
    out = pl.pallas_call(
        functools.partial(final_kernel, near * tl),
        out_shape=jax.ShapeDtypeStruct((rows, 2, ns, nsrc * per_x, n), jnp.float32),
        in_specs=[
            pl.BlockSpec(memory_space=pltpu.SMEM),
            pl.BlockSpec(memory_space=pltpu.VMEM),
        ],
        out_specs=pl.BlockSpec(memory_space=pltpu.VMEM),
        compiler_params=small(4),
        name="final",
    )(wanted, home)
    return out.transpose(0, 1, 2, 4, 3)


def solution(mesh):
    shape = dict(mesh.shape)
    cut = (shape["job"], shape["ta"] // NEAR, NEAR, shape["xyz"], shape["src"])
    mesh = Mesh(mesh.devices.reshape(cut), ("job", *TA, "xyz", "src"))
    in_specs = (
        P("src", TA, None, "job", None, "xyz"),
        P(TA, "job", None, None, "xyz"),
        P(),
        P("src"),
    )
    out_specs = P(TA, None, "job", "src", "xyz")
    return jax.shard_map(local, mesh=mesh, in_specs=in_specs, out_specs=out_specs, check_vma=False)
```

```python
import functools

import jax
import jax.numpy as jnp
from jax import lax
from jax.experimental import pallas as pl
from jax.experimental.pallas import tpu as pltpu
from jax.sharding import Mesh
from jax.sharding import PartitionSpec as P


LANES = 128


def rank_of(keys):
    extent = keys.shape[0]
    index = jnp.arange(extent, dtype=jnp.int32)
    before = (keys[None, :] < keys[:, None]) | (
        (keys[None, :] == keys[:, None]) & (index[None, :] < index[:, None])
    )
    return jnp.sum(before.astype(jnp.int32), axis=1)


def inverse_of(rank):
    extent = rank.shape[0]
    index = jnp.arange(extent, dtype=jnp.int32)
    hit = rank[None, :] == index[:, None]
    return jnp.sum(jnp.where(hit, index[None, :], 0), axis=1)


def small(mib):
    return pltpu.CompilerParams(vmem_limit_bytes=mib << 20)


def share_kernel(core_ref, in_ref, out_ref, held, packed, sem, out_sem):
    rows, parts, folds, _, per_x, nc, _, sites = in_ref.shape
    core = core_ref[0]
    copies = [
        pltpu.make_async_copy(
            in_ref.at[r, i, :, core], held.at[r * parts + i], sem.at[r * parts + i]
        )
        for r in range(rows)
        for i in range(parts)
    ]
    for copy in copies:
        copy.start()
    lines = out_ref.shape[1] // rows
    sends = []
    for r in range(rows):
        line = r * lines
        for i in range(parts):
            p = r * parts + i
            copies[p].wait()
            for c in range(nc):
                for lane in range(0, sites, LANES):
                    for f in range(folds):
                        value = held[p, f, :, c, :, lane : lane + LANES]
                        packed[f * per_x : (f + 1) * per_x, line : line + 2, :] = value
                    line += 2
        span = pl.ds(r * lines, lines)
        sends.append(
            pltpu.make_async_copy(packed.at[:, span], out_ref.at[:, span], out_sem.at[r])
        )
        sends[-1].start()
    for send in sends:
        send.wait()


def pick_rows_kernel(index_ref, table_ref, out_ref, sem):
    count = out_ref.shape[0]
    copies = [
        pltpu.make_async_copy(table_ref.at[index_ref[i]], out_ref.at[i], sem.at[i])
        for i in range(count)
    ]
    for copy in copies:
        copy.start()
    for copy in copies:
        copy.wait()


def pick_rows(table, index):
    count = index.shape[0]
    return pl.pallas_call(
        pick_rows_kernel,
        out_shape=jax.ShapeDtypeStruct((count, *table.shape[1:]), table.dtype),
        in_specs=[
            pl.BlockSpec(memory_space=pltpu.SMEM),
            pl.BlockSpec(memory_space=pltpu.VMEM),
        ],
        out_specs=pl.BlockSpec(memory_space=pl.ANY),
        scratch_shapes=[pltpu.SemaphoreType.DMA((count,))],
        compiler_params=small(4),
        name="pick_rows",
    )(index, table)


def halves(x):
    high = x.astype(jnp.bfloat16)
    low = (x - high.astype(jnp.float32)).astype(jnp.bfloat16)
    return high, low


def product_kernel(
    parts, core_ref, v_in, hh, hl, oh, ol, out_hbm,
    v_ref, p_hi, p_lo, a_ref, b_ref, out_ref, sem, v_sem, out_sem,
):
    tl, nq, nx, nsrc, piece, width = out_ref.shape
    cols = p_hi.shape[3] // LANES
    half = a_ref.shape[1] // 4
    nz = half // parts
    core = core_ref[0]

    v_copy = pltpu.make_async_copy(v_in, v_ref, v_sem)
    v_copy.start()
    copies = []
    for t in range(tl):
        for own, other, dst in ((hh, oh, p_hi), (hl, ol, p_lo)):
            pair = []
            for i, (src, slot) in enumerate(((own, core), (other, nsrc - 1 - core))):
                span = pl.ds(pl.multiple_of(slot * width, width), width)
                pair.append(
                    pltpu.make_async_copy(src.at[t], dst.at[t, :, span], sem.at[len(copies), i])
                )
                pair[-1].start()
            copies.append(pair)

    def dot(left, right):
        return lax.dot_general(
            left, right, (((1,), (1,)), ((), ())), preferred_element_type=jnp.float32
        )

    stride = tl * parts * cols * 2
    per = half // nx
    sends = []
    v_copy.wait()
    for t in range(tl):
        for i in range(parts):
            for b in range(cols):
                start = ((t * parts + i) * cols + b) * 2
                real_hi, real_lo = halves(v_ref[pl.ds(start, nz, stride=stride), :])
                imag_hi, imag_lo = halves(v_ref[pl.ds(start + 1, nz, stride=stride), :])
                lane = pl.ds(b * LANES, LANES)
                for j, (real, imag) in enumerate(((real_hi, imag_hi), (real_lo, imag_lo))):
                    top = pl.ds(2 * j * half + i * nz, nz)
                    low = pl.ds((2 * j + 1) * half + i * nz, nz)
                    a_ref[t, top, lane] = real
                    a_ref[t, low, lane] = -imag
                    b_ref[t, top, lane] = imag
                    b_ref[t, low, lane] = real
    for t in range(tl):
        for copy in copies[2 * t]:
            copy.wait()
        both = dot(a_ref[t], p_hi[t, 0]) + dot(b_ref[t], p_hi[t, 1])
        for copy in copies[2 * t + 1]:
            copy.wait()
        total = both[: 2 * half] + both[2 * half :]
        total += dot(a_ref[t, : 2 * half], p_lo[t, 0]) + dot(b_ref[t, : 2 * half], p_lo[t, 1])
        for q in range(nq):
            ri, part = divmod(q, nq // 2)
            for x in range(nx):
                first = ri * half + x * per + part * piece
                for slot in range(nsrc):
                    out_ref[t, q, x, slot] = total[
                        first : first + piece, slot * width : (slot + 1) * width
                    ]
        sends.append(pltpu.make_async_copy(out_ref.at[t], out_hbm.at[:, :, :, t], out_sem.at[t]))
        sends[-1].start()
    for send in sends:
        send.wait()


def sum_kernel(index_ref, in_ref, out_ref, held):
    near, nx, nsrc, tl = in_ref.shape[:4]
    for z in range(near):
        total = in_ref[z, 0]
        for x in range(1, nx):
            total += in_ref[z, x]
        for t in range(tl):
            for core in range(nsrc):
                held[z * tl + t, core] = total[core, t]
    for row in range(out_ref.shape[0]):
        out_ref[row] = held[index_ref[row]]


def final_kernel(per_group, order_ref, in_ref, out_ref):
    _, nq, rows, nsrc, piece, _ = in_ref.shape
    ns, n = out_ref.shape[2], out_ref.shape[4]
    parts = nq // 2
    for row in range(rows):
        group = order_ref[row] // per_group
        for core in range(nsrc):
            for ri in range(2):
                for part in range(parts):
                    value = in_ref[group, ri * parts + part, row, core]
                    first = (core * parts + part) * piece
                    for s in range(ns):
                        out_ref[row, ri, s, first : first + piece, :] = value[
                            :, s * n : (s + 1) * n
                        ]


TA = ("tq", "tp")
NEAR = 2


def local(spinors, eigvecs, group_of, source_ids):
    nta, nx, nsrc = lax.axis_size(TA), lax.axis_size("xyz"), lax.axis_size("src")
    near = lax.axis_size("tp")
    core = lax.axis_index("src").astype(jnp.int32)
    ta = lax.axis_index(TA).astype(jnp.int32)
    rows, k, _, nc, sites = eigvecs.shape
    n, tl, _, ns = spinors.shape[:4]
    mine = k // nsrc
    part = mine // nta
    per_x = mine // nx
    fold = nta // per_x

    rank = rank_of(group_of)
    ordering = inverse_of(rank)

    tail = (nc, 2, sites)
    lines = part * nc * 2 * sites // LANES
    share = pl.pallas_call(
        share_kernel,
        out_shape=jax.ShapeDtypeStruct((nta, lines * rows, LANES), jnp.float32),
        in_specs=[
            pl.BlockSpec(memory_space=pltpu.SMEM),
            pl.BlockSpec(memory_space=pltpu.HBM),
        ],
        out_specs=pl.BlockSpec(memory_space=pltpu.HBM),
        scratch_shapes=[
            pltpu.VMEM((rows * part, fold, per_x, *tail), jnp.float32),
            pltpu.VMEM((nta, lines * rows, LANES), jnp.float32),
            pltpu.SemaphoreType.DMA((rows * part,)),
            pltpu.SemaphoreType.DMA((rows,)),
        ],
        name="share",
    )(
        core[None],
        eigvecs.transpose(0, 1, 3, 2, 4).reshape(rows, part, fold, nsrc, per_x, *tail),
    )
    spread = lax.all_to_all(share, TA, 0, 0, tiled=True)
    picked = pick_rows(spread.reshape(nta * rows, lines, LANES), rank)
    sent = lax.all_to_all(picked.reshape(nta, tl * lines, LANES), TA, 0, 0, tiled=True)
    sent = sent.reshape(nta * tl * lines, LANES)

    inverse = inverse_of(source_ids - n * core)
    held = spinors.at[inverse].get(mode="promise_in_bounds")
    held = held.transpose(1, 2, 3, 0, 4, 5).reshape(tl, 2, ns * n, nc * sites)
    other = lax.ppermute(held, "src", [(i, nsrc - 1 - i) for i in range(nsrc)])

    vmem = pl.BlockSpec(memory_space=pltpu.VMEM)
    smem = pl.BlockSpec(memory_space=pltpu.SMEM)
    wide = nc * sites

    def split(x):
        high = lax.reduce_precision(x, 8, 7)
        return high.astype(jnp.bfloat16), (x - high).astype(jnp.bfloat16)

    piece = 2 * per_x // near
    hbm = pl.BlockSpec(memory_space=pltpu.HBM)
    pair = pl.pallas_call(
        functools.partial(product_kernel, part),
        out_shape=jax.ShapeDtypeStruct((near, nx, nsrc, tl, piece, ns * n), jnp.float32),
        in_specs=[smem] + [hbm] * 5,
        out_specs=hbm,
        scratch_shapes=[pltpu.VMEM(sent.shape, jnp.float32)]
        + [pltpu.VMEM((tl, 2, nsrc * ns * n, wide), jnp.bfloat16)] * 2
        + [pltpu.VMEM((tl, 4 * mine, wide), jnp.bfloat16)] * 2
        + [
            pltpu.VMEM((tl, near, nx, nsrc, piece, ns * n), jnp.float32),
            pltpu.SemaphoreType.DMA((2 * tl, 2)),
            pltpu.SemaphoreType.DMA,
            pltpu.SemaphoreType.DMA((tl,)),
        ],
        name="product",
    )(core[None], sent, *split(held), *split(other))

    pair = pair.reshape(near * nx * nsrc, tl, piece, ns * n)
    got = lax.all_to_all(pair, ("tp", "xyz", "src"), 0, 0, tiled=True)
    here = jnp.clip(ordering - (ta // near) * (near * tl), 0, near * tl - 1)
    back = pl.pallas_call(
        sum_kernel,
        out_shape=jax.ShapeDtypeStruct((nta * rows, nsrc, piece, ns * n), jnp.float32),
        in_specs=[smem, vmem],
        out_specs=vmem,
        scratch_shapes=[pltpu.VMEM((near * tl, nsrc, piece, ns * n), jnp.float32)],
        compiler_params=small(4),
        name="sum_over_xyz",
    )(here, got.reshape(near, nx, nsrc, tl, piece, ns * n))

    home = lax.all_to_all(back.reshape(nta, rows, nsrc, piece, ns * n), TA, 0, 0, tiled=True)
    home = home.reshape(nta // near, near, rows, nsrc, piece, ns * n)
    wanted = lax.dynamic_slice_in_dim(ordering, ta * rows, rows, 0)
    out = pl.pallas_call(
        functools.partial(final_kernel, near * tl),
        out_shape=jax.ShapeDtypeStruct((rows, 2, ns, nsrc * per_x, n), jnp.float32),
        in_specs=[
            pl.BlockSpec(memory_space=pltpu.SMEM),
            pl.BlockSpec(memory_space=pltpu.VMEM),
        ],
        out_specs=pl.BlockSpec(memory_space=pltpu.VMEM),
        compiler_params=small(4),
        name="final",
    )(wanted, home)
    return out.transpose(0, 1, 2, 4, 3)


def solution(mesh):
    shape = dict(mesh.shape)
    cut = (shape["job"], shape["ta"] // NEAR, NEAR, shape["xyz"], shape["src"])
    mesh = Mesh(mesh.devices.reshape(cut), ("job", *TA, "xyz", "src"))
    in_specs = (
        P("src", TA, None, "job", None, "xyz"),
        P(TA, "job", None, None, "xyz"),
        P(),
        P("src"),
    )
    out_specs = P(TA, None, "job", "src", "xyz")
    return jax.shard_map(local, mesh=mesh, in_specs=in_specs, out_specs=out_specs, check_vma=False)
```

```python
import functools

import jax
import jax.numpy as jnp
from jax import lax
from jax.experimental import pallas as pl
from jax.experimental.pallas import tpu as pltpu
from jax.sharding import Mesh
from jax.sharding import PartitionSpec as P


LANES = 128


def rank_of(keys):
    extent = keys.shape[0]
    index = jnp.arange(extent, dtype=jnp.int32)
    before = (keys[None, :] < keys[:, None]) | (
        (keys[None, :] == keys[:, None]) & (index[None, :] < index[:, None])
    )
    return jnp.sum(before.astype(jnp.int32), axis=1)


def inverse_of(rank):
    extent = rank.shape[0]
    index = jnp.arange(extent, dtype=jnp.int32)
    hit = rank[None, :] == index[:, None]
    return jnp.sum(jnp.where(hit, index[None, :], 0), axis=1)


def small(mib):
    return pltpu.CompilerParams(vmem_limit_bytes=mib << 20)


def share_kernel(core_ref, in_ref, out_ref, held, packed, sem, out_sem):
    rows, parts, folds, _, per_x, nc, _, sites = in_ref.shape
    core = core_ref[0]
    copies = [
        pltpu.make_async_copy(
            in_ref.at[r, i, :, core], held.at[r * parts + i], sem.at[r * parts + i]
        )
        for r in range(rows)
        for i in range(parts)
    ]
    for copy in copies:
        copy.start()
    lines = out_ref.shape[1] // rows
    sends = []
    for r in range(rows):
        line = r * lines
        for i in range(parts):
            p = r * parts + i
            copies[p].wait()
            for c in range(nc):
                for lane in range(0, sites, LANES):
                    for f in range(folds):
                        value = held[p, f, :, c, :, lane : lane + LANES]
                        packed[f * per_x : (f + 1) * per_x, line : line + 2, :] = value
                    line += 2
        span = pl.ds(r * lines, lines)
        sends.append(
            pltpu.make_async_copy(packed.at[:, span], out_ref.at[:, span], out_sem.at[r])
        )
        sends[-1].start()
    for send in sends:
        send.wait()


def pick_rows_kernel(index_ref, table_ref, out_ref, sem):
    count = out_ref.shape[0]
    copies = [
        pltpu.make_async_copy(table_ref.at[index_ref[i]], out_ref.at[i], sem.at[i])
        for i in range(count)
    ]
    for copy in copies:
        copy.start()
    for copy in copies:
        copy.wait()


def pick_rows(table, index):
    count = index.shape[0]
    return pl.pallas_call(
        pick_rows_kernel,
        out_shape=jax.ShapeDtypeStruct((count, *table.shape[1:]), table.dtype),
        in_specs=[
            pl.BlockSpec(memory_space=pltpu.SMEM),
            pl.BlockSpec(memory_space=pltpu.VMEM),
        ],
        out_specs=pl.BlockSpec(memory_space=pl.ANY),
        scratch_shapes=[pltpu.SemaphoreType.DMA((count,))],
        compiler_params=small(4),
        name="pick_rows",
    )(index, table)


def halves(x):
    high = x.astype(jnp.bfloat16)
    low = (x - high.astype(jnp.float32)).astype(jnp.bfloat16)
    return high, low


def split_kernel(core_ref, own_ref, other_ref, *outs):
    tl, _, width, _ = own_ref.shape
    core = core_ref[0]
    for slot, ref in ((core, own_ref), (1 - core, other_ref)):
        span = pl.ds(pl.multiple_of(slot * width, width), width)
        for t in range(tl):
            for ri in range(2):
                high, low = halves(ref[t, ri])
                outs[t][ri, span, :] = high
                outs[tl + t][ri, span, :] = low


def product_kernel(parts, tl, v_ref, *refs):
    p_hi, p_lo = refs[:tl], refs[tl : 2 * tl]
    out_hbm, a_ref, b_ref, out_ref, out_sem = refs[2 * tl :]
    _, nq, nx, nsrc, piece, width = out_ref.shape
    cols = p_hi[0].shape[2] // LANES
    half = a_ref.shape[1] // 4
    nz = half // parts

    def dot(left, right):
        return lax.dot_general(
            left, right, (((1,), (1,)), ((), ())), preferred_element_type=jnp.float32
        )

    stride = tl * parts * cols * 2
    per = half // nx
    sends = []
    for t in range(tl):
        for i in range(parts):
            for b in range(cols):
                start = ((t * parts + i) * cols + b) * 2
                real_hi, real_lo = halves(v_ref[pl.ds(start, nz, stride=stride), :])
                imag_hi, imag_lo = halves(v_ref[pl.ds(start + 1, nz, stride=stride), :])
                lane = pl.ds(b * LANES, LANES)
                for j, (real, imag) in enumerate(((real_hi, imag_hi), (real_lo, imag_lo))):
                    top = pl.ds(2 * j * half + i * nz, nz)
                    low = pl.ds((2 * j + 1) * half + i * nz, nz)
                    a_ref[t, top, lane] = real
                    a_ref[t, low, lane] = -imag
                    b_ref[t, top, lane] = imag
                    b_ref[t, low, lane] = real
        both = dot(a_ref[t], p_hi[t][0]) + dot(b_ref[t], p_hi[t][1])
        total = both[: 2 * half] + both[2 * half :]
        total += dot(a_ref[t, : 2 * half], p_lo[t][0]) + dot(b_ref[t, : 2 * half], p_lo[t][1])
        for q in range(nq):
            ri, part = divmod(q, nq // 2)
            for x in range(nx):
                first = ri * half + x * per + part * piece
                for slot in range(nsrc):
                    out_ref[t, q, x, slot] = total[
                        first : first + piece, slot * width : (slot + 1) * width
                    ]
        sends.append(pltpu.make_async_copy(out_ref.at[t], out_hbm.at[:, :, :, t], out_sem.at[t]))
        sends[-1].start()
    for send in sends:
        send.wait()


def sum_kernel(index_ref, in_ref, out_ref, held):
    near, nx, nsrc, tl = in_ref.shape[:4]
    for z in range(near):
        total = in_ref[z, 0]
        for x in range(1, nx):
            total += in_ref[z, x]
        for t in range(tl):
            for core in range(nsrc):
                held[z * tl + t, core] = total[core, t]
    for row in range(out_ref.shape[0]):
        out_ref[row] = held[index_ref[row]]


def final_kernel(per_group, order_ref, in_ref, out_ref):
    _, nq, rows, nsrc, piece, _ = in_ref.shape
    ns, n = out_ref.shape[2], out_ref.shape[4]
    parts = nq // 2
    for row in range(rows):
        group = order_ref[row] // per_group
        for core in range(nsrc):
            for ri in range(2):
                for part in range(parts):
                    value = in_ref[group, ri * parts + part, row, core]
                    first = (core * parts + part) * piece
                    for s in range(ns):
                        out_ref[row, ri, s, first : first + piece, :] = value[
                            :, s * n : (s + 1) * n
                        ]


TA = ("tq", "tp")
NEAR = 4


def local(spinors, eigvecs, group_of, source_ids):
    nta, nx, nsrc = lax.axis_size(TA), lax.axis_size("xyz"), lax.axis_size("src")
    near = lax.axis_size("tp")
    core = lax.axis_index("src").astype(jnp.int32)
    ta = lax.axis_index(TA).astype(jnp.int32)
    rows, k, _, nc, sites = eigvecs.shape
    n, tl, _, ns = spinors.shape[:4]
    mine = k // nsrc
    part = mine // nta
    per_x = mine // nx
    fold = nta // per_x

    rank = rank_of(group_of)
    ordering = inverse_of(rank)

    tail = (nc, 2, sites)
    lines = part * nc * 2 * sites // LANES
    share = pl.pallas_call(
        share_kernel,
        out_shape=jax.ShapeDtypeStruct((nta, lines * rows, LANES), jnp.float32),
        in_specs=[
            pl.BlockSpec(memory_space=pltpu.SMEM),
            pl.BlockSpec(memory_space=pltpu.HBM),
        ],
        out_specs=pl.BlockSpec(memory_space=pltpu.HBM),
        scratch_shapes=[
            pltpu.VMEM((rows * part, fold, per_x, *tail), jnp.float32),
            pltpu.VMEM((nta, lines * rows, LANES), jnp.float32),
            pltpu.SemaphoreType.DMA((rows * part,)),
            pltpu.SemaphoreType.DMA((rows,)),
        ],
        name="share",
    )(
        core[None],
        eigvecs.transpose(0, 1, 3, 2, 4).reshape(rows, part, fold, nsrc, per_x, *tail),
    )
    spread = lax.all_to_all(share, TA, 0, 0, tiled=True)
    picked = pick_rows(spread.reshape(nta * rows, lines, LANES), rank)
    sent = lax.all_to_all(picked.reshape(nta, tl * lines, LANES), TA, 0, 0, tiled=True)
    sent = sent.reshape(nta * tl * lines, LANES)

    inverse = inverse_of(source_ids - n * core)
    held = spinors.at[inverse].get(mode="promise_in_bounds")
    held = held.transpose(1, 2, 3, 0, 4, 5).reshape(tl, 2, ns * n, nc * sites)
    other = lax.ppermute(held, "src", [(i, nsrc - 1 - i) for i in range(nsrc)])

    vmem = pl.BlockSpec(memory_space=pltpu.VMEM)
    smem = pl.BlockSpec(memory_space=pltpu.SMEM)
    wide = nc * sites
    cut = pl.pallas_call(
        split_kernel,
        out_shape=[pltpu.VMEM((2, nsrc * ns * n, wide), jnp.bfloat16)] * (2 * tl),
        in_specs=[smem, vmem, vmem],
        out_specs=[vmem] * (2 * tl),
        compiler_params=small(60),
        name="split",
    )(core[None], held, other)

    piece = 2 * per_x // near
    pair = pl.pallas_call(
        functools.partial(product_kernel, part, tl),
        out_shape=jax.ShapeDtypeStruct((near, nx, nsrc, tl, piece, ns * n), jnp.float32),
        in_specs=[vmem] * (1 + 2 * tl),
        out_specs=pl.BlockSpec(memory_space=pltpu.HBM),
        scratch_shapes=[pltpu.VMEM((tl, 4 * mine, wide), jnp.bfloat16)] * 2
        + [
            pltpu.VMEM((tl, near, nx, nsrc, piece, ns * n), jnp.float32),
            pltpu.SemaphoreType.DMA((tl,)),
        ],
        compiler_params=small(12),
        name="product",
    )(sent, *cut)

    pair = pair.reshape(near * nx * nsrc, tl, piece, ns * n)
    got = lax.all_to_all(pair, ("tp", "xyz", "src"), 0, 0, tiled=True)
    here = jnp.clip(ordering - (ta // near) * (near * tl), 0, near * tl - 1)
    back = pl.pallas_call(
        sum_kernel,
        out_shape=jax.ShapeDtypeStruct((nta * rows, nsrc, piece, ns * n), jnp.float32),
        in_specs=[smem, vmem],
        out_specs=vmem,
        scratch_shapes=[pltpu.VMEM((near * tl, nsrc, piece, ns * n), jnp.float32)],
        compiler_params=small(4),
        name="sum_over_xyz",
    )(here, got.reshape(near, nx, nsrc, tl, piece, ns * n))

    home = lax.all_to_all(back.reshape(nta, rows, nsrc, piece, ns * n), TA, 0, 0, tiled=True)
    home = home.reshape(nta // near, near, rows, nsrc, piece, ns * n)
    wanted = lax.dynamic_slice_in_dim(ordering, ta * rows, rows, 0)
    out = pl.pallas_call(
        functools.partial(final_kernel, near * tl),
        out_shape=jax.ShapeDtypeStruct((rows, 2, ns, nsrc * per_x, n), jnp.float32),
        in_specs=[
            pl.BlockSpec(memory_space=pltpu.SMEM),
            pl.BlockSpec(memory_space=pltpu.VMEM),
        ],
        out_specs=pl.BlockSpec(memory_space=pltpu.VMEM),
        compiler_params=small(4),
        name="final",
    )(wanted, home)
    return out.transpose(0, 1, 2, 4, 3)


def solution(mesh):
    shape = dict(mesh.shape)
    cut = (shape["job"], shape["ta"] // NEAR, NEAR, shape["xyz"], shape["src"])
    mesh = Mesh(mesh.devices.reshape(cut), ("job", *TA, "xyz", "src"))
    in_specs = (
        P("src", TA, None, "job", None, "xyz"),
        P(TA, "job", None, None, "xyz"),
        P(),
        P("src"),
    )
    out_specs = P(TA, None, "job", "src", "xyz")
    return jax.shard_map(local, mesh=mesh, in_specs=in_specs, out_specs=out_specs, check_vma=False)
```

```python
import functools

import jax
import jax.numpy as jnp
from jax import lax
from jax.experimental import pallas as pl
from jax.experimental.pallas import tpu as pltpu
from jax.sharding import Mesh
from jax.sharding import PartitionSpec as P


LANES = 128


def rank_of(keys):
    extent = keys.shape[0]
    index = jnp.arange(extent, dtype=jnp.int32)
    before = (keys[None, :] < keys[:, None]) | (
        (keys[None, :] == keys[:, None]) & (index[None, :] < index[:, None])
    )
    return jnp.sum(before.astype(jnp.int32), axis=1)


def inverse_of(rank):
    extent = rank.shape[0]
    index = jnp.arange(extent, dtype=jnp.int32)
    hit = rank[None, :] == index[:, None]
    return jnp.sum(jnp.where(hit, index[None, :], 0), axis=1)


def small(mib):
    return pltpu.CompilerParams(vmem_limit_bytes=mib << 20)


def share_kernel(core_ref, in_ref, out_ref, held, packed, sem, out_sem):
    rows, parts, folds, _, per_x, nc, _, sites = in_ref.shape
    core = core_ref[0]
    copies = [
        pltpu.make_async_copy(
            in_ref.at[r, i, :, core], held.at[r * parts + i], sem.at[r * parts + i]
        )
        for r in range(rows)
        for i in range(parts)
    ]
    for copy in copies:
        copy.start()
    lines = out_ref.shape[1] // rows
    sends = []
    for r in range(rows):
        line = r * lines
        for i in range(parts):
            p = r * parts + i
            copies[p].wait()
            for c in range(nc):
                for lane in range(0, sites, LANES):
                    for f in range(folds):
                        value = held[p, f, :, c, :, lane : lane + LANES]
                        packed[f * per_x : (f + 1) * per_x, line : line + 2, :] = value
                    line += 2
        span = pl.ds(r * lines, lines)
        sends.append(
            pltpu.make_async_copy(packed.at[:, span], out_ref.at[:, span], out_sem.at[r])
        )
        sends[-1].start()
    for send in sends:
        send.wait()


def pick_rows_kernel(index_ref, table_ref, out_ref, sem):
    count = out_ref.shape[0]
    copies = [
        pltpu.make_async_copy(table_ref.at[index_ref[i]], out_ref.at[i], sem.at[i])
        for i in range(count)
    ]
    for copy in copies:
        copy.start()
    for copy in copies:
        copy.wait()


def pick_rows(table, index):
    count = index.shape[0]
    return pl.pallas_call(
        pick_rows_kernel,
        out_shape=jax.ShapeDtypeStruct((count, *table.shape[1:]), table.dtype),
        in_specs=[
            pl.BlockSpec(memory_space=pltpu.SMEM),
            pl.BlockSpec(memory_space=pltpu.VMEM),
        ],
        out_specs=pl.BlockSpec(memory_space=pl.ANY),
        scratch_shapes=[pltpu.SemaphoreType.DMA((count,))],
        compiler_params=small(4),
        name="pick_rows",
    )(index, table)


def halves(x):
    high = x.astype(jnp.bfloat16)
    low = (x - high.astype(jnp.float32)).astype(jnp.bfloat16)
    return high, low


def split_kernel(in_ref, *outs):
    tl = in_ref.shape[0]
    for t in range(tl):
        for ri in range(2):
            outs[t][ri], outs[tl + t][ri] = halves(in_ref[t, ri])


def product_kernel(parts, tl, slot_ref, v_ref, *refs):
    p_hi, p_lo = refs[:tl], refs[tl : 2 * tl]
    out_hbm, a_ref, b_ref, out_ref, out_sem = refs[-5:]
    _, nq, nx, piece, _ = out_ref.shape
    cols = p_hi[0].shape[2] // LANES
    half = a_ref.shape[1] // 4
    nz = half // parts
    slot = slot_ref[0]

    def dot(left, right):
        return lax.dot_general(
            left, right, (((1,), (1,)), ((), ())), preferred_element_type=jnp.float32
        )

    stride = tl * parts * cols * 2
    per = half // nx
    sends = []
    for t in range(tl):
        for i in range(parts):
            for b in range(cols):
                start = ((t * parts + i) * cols + b) * 2
                real_hi, real_lo = halves(v_ref[pl.ds(start, nz, stride=stride), :])
                imag_hi, imag_lo = halves(v_ref[pl.ds(start + 1, nz, stride=stride), :])
                lane = pl.ds(b * LANES, LANES)
                for j, (real, imag) in enumerate(((real_hi, imag_hi), (real_lo, imag_lo))):
                    top = pl.ds(2 * j * half + i * nz, nz)
                    low = pl.ds((2 * j + 1) * half + i * nz, nz)
                    a_ref[t, top, lane] = real
                    a_ref[t, low, lane] = -imag
                    b_ref[t, top, lane] = imag
                    b_ref[t, low, lane] = real
        both = dot(a_ref[t], p_hi[t][0]) + dot(b_ref[t], p_hi[t][1])
        total = both[: 2 * half] + both[2 * half :]
        total += dot(a_ref[t, : 2 * half], p_lo[t][0]) + dot(b_ref[t, : 2 * half], p_lo[t][1])
        for q in range(nq):
            ri, part = divmod(q, nq // 2)
            for x in range(nx):
                first = ri * half + x * per + part * piece
                out_ref[t, q, x] = total[first : first + piece]
        sends.append(
            pltpu.make_async_copy(out_ref.at[t], out_hbm.at[:, :, slot, t], out_sem.at[t])
        )
        sends[-1].start()
    for send in sends:
        send.wait()


def sum_kernel(index_ref, in_ref, out_ref, held):
    near, nx, nsrc, tl = in_ref.shape[:4]
    for z in range(near):
        total = in_ref[z, 0]
        for x in range(1, nx):
            total += in_ref[z, x]
        for t in range(tl):
            for core in range(nsrc):
                held[z * tl + t, core] = total[core, t]
    for row in range(out_ref.shape[0]):
        out_ref[row] = held[index_ref[row]]


def final_kernel(per_group, order_ref, in_ref, out_ref):
    _, nq, rows, nsrc, piece, _ = in_ref.shape
    ns, n = out_ref.shape[2], out_ref.shape[4]
    parts = nq // 2
    for row in range(rows):
        group = order_ref[row] // per_group
        for core in range(nsrc):
            for ri in range(2):
                for part in range(parts):
                    value = in_ref[group, ri * parts + part, row, core]
                    first = (core * parts + part) * piece
                    for s in range(ns):
                        out_ref[row, ri, s, first : first + piece, :] = value[
                            :, s * n : (s + 1) * n
                        ]


TA = ("tq", "tp")
NEAR = 4


def local(spinors, eigvecs, group_of, source_ids):
    nta, nx, nsrc = lax.axis_size(TA), lax.axis_size("xyz"), lax.axis_size("src")
    near = lax.axis_size("tp")
    core = lax.axis_index("src").astype(jnp.int32)
    ta = lax.axis_index(TA).astype(jnp.int32)
    rows, k, _, nc, sites = eigvecs.shape
    n, tl, _, ns = spinors.shape[:4]
    mine = k // nsrc
    part = mine // nta
    per_x = mine // nx
    fold = nta // per_x

    rank = rank_of(group_of)
    ordering = inverse_of(rank)

    tail = (nc, 2, sites)
    lines = part * nc * 2 * sites // LANES
    share = pl.pallas_call(
        share_kernel,
        out_shape=jax.ShapeDtypeStruct((nta, lines * rows, LANES), jnp.float32),
        in_specs=[
            pl.BlockSpec(memory_space=pltpu.SMEM),
            pl.BlockSpec(memory_space=pltpu.HBM),
        ],
        out_specs=pl.BlockSpec(memory_space=pltpu.HBM),
        scratch_shapes=[
            pltpu.VMEM((rows * part, fold, per_x, *tail), jnp.float32),
            pltpu.VMEM((nta, lines * rows, LANES), jnp.float32),
            pltpu.SemaphoreType.DMA((rows * part,)),
            pltpu.SemaphoreType.DMA((rows,)),
        ],
        name="share",
    )(
        core[None],
        eigvecs.transpose(0, 1, 3, 2, 4).reshape(rows, part, fold, nsrc, per_x, *tail),
    )
    spread = lax.all_to_all(share, TA, 0, 0, tiled=True)
    picked = pick_rows(spread.reshape(nta * rows, lines, LANES), rank)
    sent = lax.all_to_all(picked.reshape(nta, tl * lines, LANES), TA, 0, 0, tiled=True)
    sent = sent.reshape(nta * tl * lines, LANES)

    inverse = inverse_of(source_ids - n * core)
    held = spinors.at[inverse].get(mode="promise_in_bounds")
    held = held.transpose(1, 2, 3, 0, 4, 5).reshape(tl, 2, ns * n, nc * sites)
    vmem = pl.BlockSpec(memory_space=pltpu.VMEM)
    smem = pl.BlockSpec(memory_space=pltpu.SMEM)
    hbm = pl.BlockSpec(memory_space=pltpu.HBM)
    wide = nc * sites
    cut = pl.pallas_call(
        split_kernel,
        out_shape=[pltpu.VMEM((2, ns * n, wide), jnp.bfloat16)] * (2 * tl),
        in_specs=[vmem],
        out_specs=[vmem] * (2 * tl),
        compiler_params=small(61),
        name="split",
    )(held)

    sent, *cut = lax.optimization_barrier((sent, *cut))

    other = lax.ppermute(sent, "src", [(i, nsrc - 1 - i) for i in range(nsrc)])
    piece = 2 * per_x // near

    def product(slot, vectors, *into):
        return pl.pallas_call(
            functools.partial(product_kernel, part, tl),
            out_shape=jax.ShapeDtypeStruct((near, nx, nsrc, tl, piece, ns * n), jnp.float32),
            in_specs=[smem] + [vmem] * (1 + 2 * tl) + [hbm] * len(into),
            out_specs=hbm,
            scratch_shapes=[pltpu.VMEM((tl, 4 * mine, wide), jnp.bfloat16)] * 2
            + [
                pltpu.VMEM((tl, near, nx, piece, ns * n), jnp.float32),
                pltpu.SemaphoreType.DMA((tl,)),
            ],
            input_output_aliases={2 + 2 * tl: 0} if into else {},
            compiler_params=small(12),
            name="product",
        )(slot[None], vectors, *cut, *into)

    pair = product(core, sent)
    pair = product(nsrc - 1 - core, other, pair)

    pair = pair.reshape(near * nx, nsrc, tl, piece, ns * n)
    got = lax.all_to_all(pair, ("tp", "xyz"), 0, 0, tiled=True)
    here = jnp.clip(ordering - (ta // near) * (near * tl), 0, near * tl - 1)
    back = pl.pallas_call(
        sum_kernel,
        out_shape=jax.ShapeDtypeStruct((nta * rows, nsrc, piece, ns * n), jnp.float32),
        in_specs=[smem, vmem],
        out_specs=vmem,
        scratch_shapes=[pltpu.VMEM((near * tl, nsrc, piece, ns * n), jnp.float32)],
        compiler_params=small(4),
        name="sum_over_xyz",
    )(here, got.reshape(near, nx, nsrc, tl, piece, ns * n))

    home = lax.all_to_all(back.reshape(nta, rows, nsrc, piece, ns * n), TA, 0, 0, tiled=True)
    home = home.reshape(nta // near, near, rows, nsrc, piece, ns * n)
    wanted = lax.dynamic_slice_in_dim(ordering, ta * rows, rows, 0)
    out = pl.pallas_call(
        functools.partial(final_kernel, near * tl),
        out_shape=jax.ShapeDtypeStruct((rows, 2, ns, nsrc * per_x, n), jnp.float32),
        in_specs=[
            pl.BlockSpec(memory_space=pltpu.SMEM),
            pl.BlockSpec(memory_space=pltpu.VMEM),
        ],
        out_specs=pl.BlockSpec(memory_space=pltpu.VMEM),
        compiler_params=small(4),
        name="final",
    )(wanted, home)
    return out.transpose(0, 1, 2, 4, 3)


def solution(mesh):
    shape = dict(mesh.shape)
    cut = (shape["job"], shape["ta"] // NEAR, NEAR, shape["xyz"], shape["src"])
    mesh = Mesh(mesh.devices.reshape(cut), ("job", *TA, "xyz", "src"))
    in_specs = (
        P("src", TA, None, "job", None, "xyz"),
        P(TA, "job", None, None, "xyz"),
        P(),
        P("src"),
    )
    out_specs = P(TA, None, "job", "src", "xyz")
    return jax.shard_map(local, mesh=mesh, in_specs=in_specs, out_specs=out_specs, check_vma=False)
```

```python
import functools

import jax
import jax.numpy as jnp
from jax import lax
from jax.experimental import pallas as pl
from jax.experimental.pallas import tpu as pltpu
from jax.sharding import Mesh
from jax.sharding import PartitionSpec as P


LANES = 128


def rank_of(keys):
    extent = keys.shape[0]
    index = jnp.arange(extent, dtype=jnp.int32)
    before = (keys[None, :] < keys[:, None]) | (
        (keys[None, :] == keys[:, None]) & (index[None, :] < index[:, None])
    )
    return jnp.sum(before.astype(jnp.int32), axis=1)


def inverse_of(rank):
    extent = rank.shape[0]
    index = jnp.arange(extent, dtype=jnp.int32)
    hit = rank[None, :] == index[:, None]
    return jnp.sum(jnp.where(hit, index[None, :], 0), axis=1)


def small(mib):
    return pltpu.CompilerParams(vmem_limit_bytes=mib << 20)


def share_kernel(core_ref, in_ref, out_ref, held, packed, sem, out_sem):
    rows, parts, folds, _, per_x, nc, _, sites = in_ref.shape
    core = core_ref[0]
    copies = [
        pltpu.make_async_copy(
            in_ref.at[r, i, :, core], held.at[r * parts + i], sem.at[r * parts + i]
        )
        for r in range(rows)
        for i in range(parts)
    ]
    for copy in copies:
        copy.start()
    lines = out_ref.shape[1] // rows
    sends = []
    for r in range(rows):
        line = r * lines
        for i in range(parts):
            p = r * parts + i
            copies[p].wait()
            for c in range(nc):
                for lane in range(0, sites, LANES):
                    for f in range(folds):
                        value = held[p, f, :, c, :, lane : lane + LANES]
                        packed[f * per_x : (f + 1) * per_x, line : line + 2, :] = value
                    line += 2
        span = pl.ds(r * lines, lines)
        sends.append(
            pltpu.make_async_copy(packed.at[:, span], out_ref.at[:, span], out_sem.at[r])
        )
        sends[-1].start()
    for send in sends:
        send.wait()


def pick_rows_kernel(index_ref, table_ref, out_ref, sem):
    count = out_ref.shape[0]
    copies = [
        pltpu.make_async_copy(table_ref.at[index_ref[i]], out_ref.at[i], sem.at[i])
        for i in range(count)
    ]
    for copy in copies:
        copy.start()
    for copy in copies:
        copy.wait()


def pick_rows(table, index):
    count = index.shape[0]
    return pl.pallas_call(
        pick_rows_kernel,
        out_shape=jax.ShapeDtypeStruct((count, *table.shape[1:]), table.dtype),
        in_specs=[
            pl.BlockSpec(memory_space=pltpu.SMEM),
            pl.BlockSpec(memory_space=pltpu.VMEM),
        ],
        out_specs=pl.BlockSpec(memory_space=pl.ANY),
        scratch_shapes=[pltpu.SemaphoreType.DMA((count,))],
        compiler_params=small(4),
        name="pick_rows",
    )(index, table)


def halves(x):
    high = x.astype(jnp.bfloat16)
    low = (x - high.astype(jnp.float32)).astype(jnp.bfloat16)
    return high, low


def split_kernel(core_ref, own_ref, other_ref, *outs):
    tl, _, width, _ = own_ref.shape
    core = core_ref[0]
    for slot, ref in ((core, own_ref), (1 - core, other_ref)):
        span = pl.ds(pl.multiple_of(slot * width, width), width)
        for t in range(tl):
            for ri in range(2):
                high, low = halves(ref[t, ri])
                outs[t][ri, span, :] = high
                outs[tl + t][ri, span, :] = low


def product_kernel(parts, tl, v_ref, *refs):
    p_hi, p_lo = refs[:tl], refs[tl : 2 * tl]
    out_ref, a_ref, b_ref = refs[2 * tl :]
    nq, nx, nsrc, _, piece, width = out_ref.shape
    cols = p_hi[0].shape[2] // LANES
    half = a_ref.shape[1] // 4
    nz = half // parts

    def dot(left, right):
        return lax.dot_general(
            left, right, (((1,), (1,)), ((), ())), preferred_element_type=jnp.float32
        )

    stride = tl * parts * cols * 2
    per = half // nx
    for t in range(tl):
        for i in range(parts):
            for b in range(cols):
                start = ((t * parts + i) * cols + b) * 2
                real_hi, real_lo = halves(v_ref[pl.ds(start, nz, stride=stride), :])
                imag_hi, imag_lo = halves(v_ref[pl.ds(start + 1, nz, stride=stride), :])
                lane = pl.ds(b * LANES, LANES)
                for j, (real, imag) in enumerate(((real_hi, imag_hi), (real_lo, imag_lo))):
                    top = pl.ds(2 * j * half + i * nz, nz)
                    low = pl.ds((2 * j + 1) * half + i * nz, nz)
                    a_ref[t, top, lane] = real
                    a_ref[t, low, lane] = -imag
                    b_ref[t, top, lane] = imag
                    b_ref[t, low, lane] = real
        both = dot(a_ref[t], p_hi[t][0]) + dot(b_ref[t], p_hi[t][1])
        total = both[: 2 * half] + both[2 * half :]
        total += dot(a_ref[t, : 2 * half], p_lo[t][0]) + dot(b_ref[t, : 2 * half], p_lo[t][1])
        for q in range(nq):
            ri, part = divmod(q, nq // 2)
            for x in range(nx):
                first = ri * half + x * per + part * piece
                for slot in range(nsrc):
                    out_ref[q, x, slot, t] = total[
                        first : first + piece, slot * width : (slot + 1) * width
                    ]


def sum_kernel(index_ref, in_ref, out_ref, held):
    near, nx, nsrc, tl = in_ref.shape[:4]
    for z in range(near):
        total = in_ref[z, 0]
        for x in range(1, nx):
            total += in_ref[z, x]
        for t in range(tl):
            for core in range(nsrc):
                held[z * tl + t, core] = total[core, t]
    for row in range(out_ref.shape[0]):
        out_ref[row] = held[index_ref[row]]


def final_kernel(per_group, order_ref, in_ref, out_ref):
    _, nq, rows, nsrc, piece, _ = in_ref.shape
    ns, n = out_ref.shape[2], out_ref.shape[4]
    parts = nq // 2
    for row in range(rows):
        group = order_ref[row] // per_group
        for core in range(nsrc):
            for ri in range(2):
                for part in range(parts):
                    value = in_ref[group, ri * parts + part, row, core]
                    first = (core * parts + part) * piece
                    for s in range(ns):
                        out_ref[row, ri, s, first : first + piece, :] = value[
                            :, s * n : (s + 1) * n
                        ]


TA = ("tq", "tp")
NEAR = 4


def local(spinors, eigvecs, group_of, source_ids):
    nta, nx, nsrc = lax.axis_size(TA), lax.axis_size("xyz"), lax.axis_size("src")
    near = lax.axis_size("tp")
    core = lax.axis_index("src").astype(jnp.int32)
    ta = lax.axis_index(TA).astype(jnp.int32)
    rows, k, _, nc, sites = eigvecs.shape
    n, tl, _, ns = spinors.shape[:4]
    mine = k // nsrc
    part = mine // nta
    per_x = mine // nx
    fold = nta // per_x

    rank = rank_of(group_of)
    ordering = inverse_of(rank)

    tail = (nc, 2, sites)
    lines = part * nc * 2 * sites // LANES
    share = pl.pallas_call(
        share_kernel,
        out_shape=jax.ShapeDtypeStruct((nta, lines * rows, LANES), jnp.float32),
        in_specs=[
            pl.BlockSpec(memory_space=pltpu.SMEM),
            pl.BlockSpec(memory_space=pltpu.HBM),
        ],
        out_specs=pl.BlockSpec(memory_space=pltpu.HBM),
        scratch_shapes=[
            pltpu.VMEM((rows * part, fold, per_x, *tail), jnp.float32),
            pltpu.VMEM((nta, lines * rows, LANES), jnp.float32),
            pltpu.SemaphoreType.DMA((rows * part,)),
            pltpu.SemaphoreType.DMA((rows,)),
        ],
        name="share",
    )(
        core[None],
        eigvecs.transpose(0, 1, 3, 2, 4).reshape(rows, part, fold, nsrc, per_x, *tail),
    )
    spread = lax.all_to_all(share, TA, 0, 0, tiled=True)
    inverse = inverse_of(source_ids - n * core)
    held = spinors.at[inverse].get(mode="promise_in_bounds")
    held = held.transpose(1, 2, 3, 0, 4, 5).reshape(tl, 2, ns * n, nc * sites)
    other = lax.ppermute(held, "src", [(i, nsrc - 1 - i) for i in range(nsrc)])

    vmem = pl.BlockSpec(memory_space=pltpu.VMEM)
    smem = pl.BlockSpec(memory_space=pltpu.SMEM)
    wide = nc * sites
    cut = pl.pallas_call(
        split_kernel,
        out_shape=[pltpu.VMEM((2, nsrc * ns * n, wide), jnp.bfloat16)] * (2 * tl),
        in_specs=[smem, vmem, vmem],
        out_specs=[vmem] * (2 * tl),
        compiler_params=small(60),
        name="split",
    )(core[None], held, other)

    here = jnp.clip(ordering - (ta // near) * (near * tl), 0, near * tl - 1)
    wanted = lax.dynamic_slice_in_dim(ordering, ta * rows, rows, 0)
    spread, rank, here, wanted, *cut = lax.optimization_barrier(
        (spread, rank, here, wanted, *cut)
    )

    picked = pick_rows(spread.reshape(nta * rows, lines, LANES), rank)
    sent = lax.all_to_all(picked.reshape(nta, tl * lines, LANES), TA, 0, 0, tiled=True)
    sent = sent.reshape(nta * tl * lines, LANES)

    piece = 2 * per_x // near
    pair = pl.pallas_call(
        functools.partial(product_kernel, part, tl),
        out_shape=jax.ShapeDtypeStruct((near, nx, nsrc, tl, piece, ns * n), jnp.float32),
        in_specs=[vmem] * (1 + 2 * tl),
        out_specs=vmem,
        scratch_shapes=[pltpu.VMEM((tl, 4 * mine, wide), jnp.bfloat16)] * 2,
        compiler_params=small(12),
        name="product",
    )(sent, *cut)

    pair = pair.reshape(near * nx * nsrc, tl, piece, ns * n)
    got = lax.all_to_all(pair, ("tp", "xyz", "src"), 0, 0, tiled=True)
    back = pl.pallas_call(
        sum_kernel,
        out_shape=jax.ShapeDtypeStruct((nta * rows, nsrc, piece, ns * n), jnp.float32),
        in_specs=[smem, vmem],
        out_specs=vmem,
        scratch_shapes=[pltpu.VMEM((near * tl, nsrc, piece, ns * n), jnp.float32)],
        compiler_params=small(4),
        name="sum_over_xyz",
    )(here, got.reshape(near, nx, nsrc, tl, piece, ns * n))

    home = lax.all_to_all(back.reshape(nta, rows, nsrc, piece, ns * n), TA, 0, 0, tiled=True)
    home = home.reshape(nta // near, near, rows, nsrc, piece, ns * n)
    out = pl.pallas_call(
        functools.partial(final_kernel, near * tl),
        out_shape=jax.ShapeDtypeStruct((rows, 2, ns, nsrc * per_x, n), jnp.float32),
        in_specs=[
            pl.BlockSpec(memory_space=pltpu.SMEM),
            pl.BlockSpec(memory_space=pltpu.VMEM),
        ],
        out_specs=pl.BlockSpec(memory_space=pltpu.VMEM),
        compiler_params=small(4),
        name="final",
    )(wanted, home)
    return out.transpose(0, 1, 2, 4, 3)


def solution(mesh):
    shape = dict(mesh.shape)
    cut = (shape["job"], shape["ta"] // NEAR, NEAR, shape["xyz"], shape["src"])
    mesh = Mesh(mesh.devices.reshape(cut), ("job", *TA, "xyz", "src"))
    in_specs = (
        P("src", TA, None, "job", None, "xyz"),
        P(TA, "job", None, None, "xyz"),
        P(),
        P("src"),
    )
    out_specs = P(TA, None, "job", "src", "xyz")
    return jax.shard_map(local, mesh=mesh, in_specs=in_specs, out_specs=out_specs, check_vma=False)
```

```python
import functools

import jax
import jax.numpy as jnp
from jax import lax
from jax.experimental import pallas as pl
from jax.experimental.pallas import tpu as pltpu
from jax.sharding import Mesh
from jax.sharding import PartitionSpec as P


LANES = 128


def rank_of(keys):
    extent = keys.shape[0]
    index = jnp.arange(extent, dtype=jnp.int32)
    before = (keys[None, :] < keys[:, None]) | (
        (keys[None, :] == keys[:, None]) & (index[None, :] < index[:, None])
    )
    return jnp.sum(before.astype(jnp.int32), axis=1)


def inverse_of(rank):
    extent = rank.shape[0]
    index = jnp.arange(extent, dtype=jnp.int32)
    hit = rank[None, :] == index[:, None]
    return jnp.sum(jnp.where(hit, index[None, :], 0), axis=1)


def small(mib):
    return pltpu.CompilerParams(vmem_limit_bytes=mib << 20)


def share_kernel(core_ref, in_ref, out_ref, held, packed, sem, out_sem):
    rows, parts, folds, _, per_x, nc, _, sites = in_ref.shape
    core = core_ref[0]
    copies = [
        pltpu.make_async_copy(
            in_ref.at[r, i, :, core], held.at[r * parts + i], sem.at[r * parts + i]
        )
        for r in range(rows)
        for i in range(parts)
    ]
    for copy in copies:
        copy.start()
    lines = out_ref.shape[1] // rows
    sends = []
    for r in range(rows):
        line = r * lines
        for i in range(parts):
            p = r * parts + i
            copies[p].wait()
            for c in range(nc):
                for lane in range(0, sites, LANES):
                    for f in range(folds):
                        value = held[p, f, :, c, :, lane : lane + LANES]
                        packed[f * per_x : (f + 1) * per_x, line : line + 2, :] = value
                    line += 2
        span = pl.ds(r * lines, lines)
        sends.append(
            pltpu.make_async_copy(packed.at[:, span], out_ref.at[:, span], out_sem.at[r])
        )
        sends[-1].start()
    for send in sends:
        send.wait()


def pick_rows_kernel(index_ref, table_ref, out_ref):
    for i in range(out_ref.shape[0]):
        out_ref[i] = table_ref[index_ref[i]]


def pick_rows(table, index):
    count = index.shape[0]
    return pl.pallas_call(
        pick_rows_kernel,
        out_shape=jax.ShapeDtypeStruct((count, *table.shape[1:]), table.dtype),
        in_specs=[
            pl.BlockSpec(memory_space=pltpu.SMEM),
            pl.BlockSpec(memory_space=pltpu.VMEM),
        ],
        out_specs=pl.BlockSpec(memory_space=pltpu.VMEM),
        compiler_params=small(4),
        name="pick_rows",
    )(index, table)


def halves(x):
    high = x.astype(jnp.bfloat16)
    low = (x - high.astype(jnp.float32)).astype(jnp.bfloat16)
    return high, low


def split_kernel(core_ref, own_ref, other_ref, *outs):
    tl, _, width, _ = own_ref.shape
    core = core_ref[0]
    for slot, ref in ((core, own_ref), (1 - core, other_ref)):
        span = pl.ds(pl.multiple_of(slot * width, width), width)
        for t in range(tl):
            for ri in range(2):
                high, low = halves(ref[t, ri])
                outs[t][ri, span, :] = high
                outs[tl + t][ri, span, :] = low


def product_kernel(parts, tl, v_ref, *refs):
    p_hi, p_lo = refs[:tl], refs[tl : 2 * tl]
    out_ref, a_ref, b_ref = refs[2 * tl :]
    nq, nx, nsrc, _, piece, width = out_ref.shape
    cols = p_hi[0].shape[2] // LANES
    half = a_ref.shape[1] // 4
    nz = half // parts

    def dot(left, right):
        return lax.dot_general(
            left, right, (((1,), (1,)), ((), ())), preferred_element_type=jnp.float32
        )

    stride = tl * parts * cols * 2
    per = half // nx
    for t in range(tl):
        for i in range(parts):
            for b in range(cols):
                start = ((t * parts + i) * cols + b) * 2
                real_hi, real_lo = halves(v_ref[pl.ds(start, nz, stride=stride), :])
                imag_hi, imag_lo = halves(v_ref[pl.ds(start + 1, nz, stride=stride), :])
                lane = pl.ds(b * LANES, LANES)
                for j, (real, imag) in enumerate(((real_hi, imag_hi), (real_lo, imag_lo))):
                    top = pl.ds(2 * j * half + i * nz, nz)
                    low = pl.ds((2 * j + 1) * half + i * nz, nz)
                    a_ref[t, top, lane] = real
                    a_ref[t, low, lane] = -imag
                    b_ref[t, top, lane] = imag
                    b_ref[t, low, lane] = real
        both = dot(a_ref[t], p_hi[t][0]) + dot(b_ref[t], p_hi[t][1])
        total = both[: 2 * half] + both[2 * half :]
        total += dot(a_ref[t, : 2 * half], p_lo[t][0]) + dot(b_ref[t, : 2 * half], p_lo[t][1])
        for q in range(nq):
            ri, part = divmod(q, nq // 2)
            for x in range(nx):
                first = ri * half + x * per + part * piece
                for slot in range(nsrc):
                    out_ref[q, x, slot, t] = total[
                        first : first + piece, slot * width : (slot + 1) * width
                    ]


def sum_kernel(index_ref, in_ref, out_ref, held):
    near, nx, nsrc, tl = in_ref.shape[:4]
    for z in range(near):
        total = in_ref[z, 0]
        for x in range(1, nx):
            total += in_ref[z, x]
        for t in range(tl):
            for core in range(nsrc):
                held[z * tl + t, core] = total[core, t]
    for row in range(out_ref.shape[0]):
        out_ref[row] = held[index_ref[row]]


def final_kernel(per_group, order_ref, in_ref, out_ref):
    _, nq, rows, nsrc, piece, _ = in_ref.shape
    ns, n = out_ref.shape[2], out_ref.shape[4]
    parts = nq // 2
    for row in range(rows):
        group = order_ref[row] // per_group
        for core in range(nsrc):
            for ri in range(2):
                for part in range(parts):
                    value = in_ref[group, ri * parts + part, row, core]
                    first = (core * parts + part) * piece
                    for s in range(ns):
                        out_ref[row, ri, s, first : first + piece, :] = value[
                            :, s * n : (s + 1) * n
                        ]


TA = ("tq", "tp")
NEAR = 4


def local(spinors, eigvecs, group_of, source_ids):
    nta, nx, nsrc = lax.axis_size(TA), lax.axis_size("xyz"), lax.axis_size("src")
    near = lax.axis_size("tp")
    core = lax.axis_index("src").astype(jnp.int32)
    ta = lax.axis_index(TA).astype(jnp.int32)
    rows, k, _, nc, sites = eigvecs.shape
    n, tl, _, ns = spinors.shape[:4]
    mine = k // nsrc
    part = mine // nta
    per_x = mine // nx
    fold = nta // per_x

    rank = rank_of(group_of)
    ordering = inverse_of(rank)

    tail = (nc, 2, sites)
    lines = part * nc * 2 * sites // LANES
    share = pl.pallas_call(
        share_kernel,
        out_shape=jax.ShapeDtypeStruct((nta, lines * rows, LANES), jnp.float32),
        in_specs=[
            pl.BlockSpec(memory_space=pltpu.SMEM),
            pl.BlockSpec(memory_space=pltpu.HBM),
        ],
        out_specs=pl.BlockSpec(memory_space=pltpu.HBM),
        scratch_shapes=[
            pltpu.VMEM((rows * part, fold, per_x, *tail), jnp.float32),
            pltpu.VMEM((nta, lines * rows, LANES), jnp.float32),
            pltpu.SemaphoreType.DMA((rows * part,)),
            pltpu.SemaphoreType.DMA((rows,)),
        ],
        name="share",
    )(
        core[None],
        eigvecs.transpose(0, 1, 3, 2, 4).reshape(rows, part, fold, nsrc, per_x, *tail),
    )
    spread = lax.all_to_all(share, TA, 0, 0, tiled=True)
    inverse = inverse_of(source_ids - n * core)
    held = spinors.at[inverse].get(mode="promise_in_bounds")
    held = held.transpose(1, 2, 3, 0, 4, 5).reshape(tl, 2, ns * n, nc * sites)
    other = lax.ppermute(held, "src", [(i, nsrc - 1 - i) for i in range(nsrc)])

    vmem = pl.BlockSpec(memory_space=pltpu.VMEM)
    smem = pl.BlockSpec(memory_space=pltpu.SMEM)
    wide = nc * sites
    cut = pl.pallas_call(
        split_kernel,
        out_shape=[pltpu.VMEM((2, nsrc * ns * n, wide), jnp.bfloat16)] * (2 * tl),
        in_specs=[smem, vmem, vmem],
        out_specs=[vmem] * (2 * tl),
        compiler_params=small(60),
        name="split",
    )(core[None], held, other)

    here = jnp.clip(ordering - (ta // near) * (near * tl), 0, near * tl - 1)
    wanted = lax.dynamic_slice_in_dim(ordering, ta * rows, rows, 0)
    spread, rank, here, wanted, *cut = lax.optimization_barrier(
        (spread, rank, here, wanted, *cut)
    )

    picked = pick_rows(spread.reshape(nta * rows, lines, LANES), rank)
    sent = lax.all_to_all(picked.reshape(nta, tl * lines, LANES), TA, 0, 0, tiled=True)
    sent = sent.reshape(nta * tl * lines, LANES)

    piece = 2 * per_x // near
    pair = pl.pallas_call(
        functools.partial(product_kernel, part, tl),
        out_shape=jax.ShapeDtypeStruct((near, nx, nsrc, tl, piece, ns * n), jnp.float32),
        in_specs=[vmem] * (1 + 2 * tl),
        out_specs=vmem,
        scratch_shapes=[pltpu.VMEM((tl, 4 * mine, wide), jnp.bfloat16)] * 2,
        compiler_params=small(12),
        name="product",
    )(sent, *cut)

    pair = pair.reshape(near * nx * nsrc, tl, piece, ns * n)
    got = lax.all_to_all(pair, ("tp", "xyz", "src"), 0, 0, tiled=True)
    back = pl.pallas_call(
        sum_kernel,
        out_shape=jax.ShapeDtypeStruct((nta * rows, nsrc, piece, ns * n), jnp.float32),
        in_specs=[smem, vmem],
        out_specs=vmem,
        scratch_shapes=[pltpu.VMEM((near * tl, nsrc, piece, ns * n), jnp.float32)],
        compiler_params=small(4),
        name="sum_over_xyz",
    )(here, got.reshape(near, nx, nsrc, tl, piece, ns * n))

    home = lax.all_to_all(back.reshape(nta, rows, nsrc, piece, ns * n), TA, 0, 0, tiled=True)
    home = home.reshape(nta // near, near, rows, nsrc, piece, ns * n)
    out = pl.pallas_call(
        functools.partial(final_kernel, near * tl),
        out_shape=jax.ShapeDtypeStruct((rows, 2, ns, nsrc * per_x, n), jnp.float32),
        in_specs=[
            pl.BlockSpec(memory_space=pltpu.SMEM),
            pl.BlockSpec(memory_space=pltpu.VMEM),
        ],
        out_specs=pl.BlockSpec(memory_space=pltpu.VMEM),
        compiler_params=small(4),
        name="final",
    )(wanted, home)
    return out.transpose(0, 1, 2, 4, 3)


def solution(mesh):
    shape = dict(mesh.shape)
    cut = (shape["job"], shape["ta"] // NEAR, NEAR, shape["xyz"], shape["src"])
    mesh = Mesh(mesh.devices.reshape(cut), ("job", *TA, "xyz", "src"))
    in_specs = (
        P("src", TA, None, "job", None, "xyz"),
        P(TA, "job", None, None, "xyz"),
        P(),
        P("src"),
    )
    out_specs = P(TA, None, "job", "src", "xyz")
    return jax.shard_map(local, mesh=mesh, in_specs=in_specs, out_specs=out_specs, check_vma=False)
```

```python
import functools

import jax
import jax.numpy as jnp
from jax import lax
from jax.experimental import pallas as pl
from jax.experimental.pallas import tpu as pltpu
from jax.sharding import Mesh
from jax.sharding import PartitionSpec as P


LANES = 128


def rank_of(keys):
    extent = keys.shape[0]
    index = jnp.arange(extent, dtype=jnp.int32)
    before = (keys[None, :] < keys[:, None]) | (
        (keys[None, :] == keys[:, None]) & (index[None, :] < index[:, None])
    )
    return jnp.sum(before.astype(jnp.int32), axis=1)


def inverse_of(rank):
    extent = rank.shape[0]
    index = jnp.arange(extent, dtype=jnp.int32)
    hit = rank[None, :] == index[:, None]
    return jnp.sum(jnp.where(hit, index[None, :], 0), axis=1)


def small(mib):
    return pltpu.CompilerParams(vmem_limit_bytes=mib << 20)


def share_kernel(core_ref, in_ref, out_ref, held, packed, sem, out_sem):
    rows, parts, folds, _, per_x, nc, _, sites = in_ref.shape
    core = core_ref[0]
    copies = [
        pltpu.make_async_copy(
            in_ref.at[r, i, :, core], held.at[r * parts + i], sem.at[r * parts + i]
        )
        for r in range(rows)
        for i in range(parts)
    ]
    for copy in copies:
        copy.start()
    lines = out_ref.shape[1] // rows
    sends = []
    for r in range(rows):
        line = r * lines
        for i in range(parts):
            p = r * parts + i
            copies[p].wait()
            for c in range(nc):
                for lane in range(0, sites, LANES):
                    for f in range(folds):
                        value = held[p, f, :, c, :, lane : lane + LANES]
                        packed[f * per_x : (f + 1) * per_x, line : line + 2, :] = value
                    line += 2
        span = pl.ds(r * lines, lines)
        sends.append(
            pltpu.make_async_copy(packed.at[:, span], out_ref.at[:, span], out_sem.at[r])
        )
        sends[-1].start()
    for send in sends:
        send.wait()


def pick_rows_kernel(index_ref, table_ref, out_ref):
    for i in range(out_ref.shape[0]):
        out_ref[i] = table_ref[index_ref[i]]


def pick_rows(table, index):
    count = index.shape[0]
    return pl.pallas_call(
        pick_rows_kernel,
        out_shape=jax.ShapeDtypeStruct((count, *table.shape[1:]), table.dtype),
        in_specs=[
            pl.BlockSpec(memory_space=pltpu.SMEM),
            pl.BlockSpec(memory_space=pltpu.VMEM),
        ],
        out_specs=pl.BlockSpec(memory_space=pltpu.VMEM),
        compiler_params=small(4),
        name="pick_rows",
    )(index, table)


def halves(x):
    high = x.astype(jnp.bfloat16)
    low = (x - high.astype(jnp.float32)).astype(jnp.bfloat16)
    return high, low


def split_kernel(core_ref, own_ref, other_ref, *outs):
    tl, _, width, _ = own_ref.shape
    core = core_ref[0]
    for slot, ref in ((core, own_ref), (1 - core, other_ref)):
        span = pl.ds(pl.multiple_of(slot * width, width), width)
        for t in range(tl):
            for ri in range(2):
                high, low = halves(ref[t, ri])
                outs[t][ri, span, :] = high
                outs[tl + t][ri, span, :] = low


def product_kernel(parts, tl, v_ref, *refs):
    p_hi, p_lo = refs[:tl], refs[tl : 2 * tl]
    out_ref, a_ref, b_ref = refs[2 * tl :]
    nq, nx, nsrc, _, piece, width = out_ref.shape
    cols = p_hi[0].shape[2] // LANES
    half = a_ref.shape[1] // 4
    nz = half // parts

    def dot(left, right):
        return lax.dot_general(
            left, right, (((1,), (1,)), ((), ())), preferred_element_type=jnp.float32
        )

    stride = tl * parts * cols * 2
    per = half // nx
    for t in range(tl):
        for i in range(parts):
            for b in range(cols):
                start = ((t * parts + i) * cols + b) * 2
                real_hi, real_lo = halves(v_ref[pl.ds(start, nz, stride=stride), :])
                imag_hi, imag_lo = halves(v_ref[pl.ds(start + 1, nz, stride=stride), :])
                lane = pl.ds(b * LANES, LANES)
                for j, (real, imag) in enumerate(((real_hi, imag_hi), (real_lo, imag_lo))):
                    top = pl.ds(2 * j * half + i * nz, nz)
                    low = pl.ds((2 * j + 1) * half + i * nz, nz)
                    a_ref[t, top, lane] = real
                    a_ref[t, low, lane] = -imag
                    b_ref[t, top, lane] = imag
                    b_ref[t, low, lane] = real
        both = dot(a_ref[t], p_hi[t][0]) + dot(b_ref[t], p_hi[t][1])
        total = both[: 2 * half] + both[2 * half :]
        total += dot(a_ref[t, : 2 * half], p_lo[t][0]) + dot(b_ref[t, : 2 * half], p_lo[t][1])
        for q in range(nq):
            ri, part = divmod(q, nq // 2)
            for x in range(nx):
                first = ri * half + x * per + part * piece
                for slot in range(nsrc):
                    out_ref[q, x, slot, t] = total[
                        first : first + piece, slot * width : (slot + 1) * width
                    ]


def sum_kernel(index_ref, in_ref, out_ref, held):
    near, nx, nsrc, tl = in_ref.shape[:4]
    for z in range(near):
        total = in_ref[z, 0]
        for x in range(1, nx):
            total += in_ref[z, x]
        for t in range(tl):
            for core in range(nsrc):
                held[z * tl + t, core] = total[core, t]
    for row in range(out_ref.shape[0]):
        out_ref[row] = held[index_ref[row]]


def final_kernel(per_group, order_ref, in_ref, out_ref):
    _, nq, rows, nsrc, piece, _ = in_ref.shape
    ns, n = out_ref.shape[2], out_ref.shape[4]
    parts = nq // 2
    for row in range(rows):
        group = order_ref[row] // per_group
        for core in range(nsrc):
            for ri in range(2):
                for part in range(parts):
                    value = in_ref[group, ri * parts + part, row, core]
                    first = (core * parts + part) * piece
                    for s in range(ns):
                        out_ref[row, ri, s, first : first + piece, :] = value[
                            :, s * n : (s + 1) * n
                        ]


TA = ("tq", "tp")
NEAR = 2


def local(spinors, eigvecs, group_of, source_ids):
    nta, nx, nsrc = lax.axis_size(TA), lax.axis_size("xyz"), lax.axis_size("src")
    near = lax.axis_size("tp")
    core = lax.axis_index("src").astype(jnp.int32)
    ta = lax.axis_index(TA).astype(jnp.int32)
    rows, k, _, nc, sites = eigvecs.shape
    n, tl, _, ns = spinors.shape[:4]
    mine = k // nsrc
    part = mine // nta
    per_x = mine // nx
    fold = nta // per_x

    rank = rank_of(group_of)
    ordering = inverse_of(rank)

    tail = (nc, 2, sites)
    lines = part * nc * 2 * sites // LANES
    share = pl.pallas_call(
        share_kernel,
        out_shape=jax.ShapeDtypeStruct((nta, lines * rows, LANES), jnp.float32),
        in_specs=[
            pl.BlockSpec(memory_space=pltpu.SMEM),
            pl.BlockSpec(memory_space=pltpu.HBM),
        ],
        out_specs=pl.BlockSpec(memory_space=pltpu.HBM),
        scratch_shapes=[
            pltpu.VMEM((rows * part, fold, per_x, *tail), jnp.float32),
            pltpu.VMEM((nta, lines * rows, LANES), jnp.float32),
            pltpu.SemaphoreType.DMA((rows * part,)),
            pltpu.SemaphoreType.DMA((rows,)),
        ],
        name="share",
    )(
        core[None],
        eigvecs.transpose(0, 1, 3, 2, 4).reshape(rows, part, fold, nsrc, per_x, *tail),
    )
    spread = lax.all_to_all(share, TA, 0, 0, tiled=True)
    inverse = inverse_of(source_ids - n * core)
    held = spinors.at[inverse].get(mode="promise_in_bounds")
    held = held.transpose(1, 2, 3, 0, 4, 5).reshape(tl, 2, ns * n, nc * sites)
    other = lax.ppermute(held, "src", [(i, nsrc - 1 - i) for i in range(nsrc)])

    vmem = pl.BlockSpec(memory_space=pltpu.VMEM)
    smem = pl.BlockSpec(memory_space=pltpu.SMEM)
    wide = nc * sites
    cut = pl.pallas_call(
        split_kernel,
        out_shape=[pltpu.VMEM((2, nsrc * ns * n, wide), jnp.bfloat16)] * (2 * tl),
        in_specs=[smem, vmem, vmem],
        out_specs=[vmem] * (2 * tl),
        compiler_params=small(60),
        name="split",
    )(core[None], held, other)

    here = jnp.clip(ordering - (ta // near) * (near * tl), 0, near * tl - 1)
    wanted = lax.dynamic_slice_in_dim(ordering, ta * rows, rows, 0)
    spread, rank, here, wanted, *cut = lax.optimization_barrier(
        (spread, rank, here, wanted, *cut)
    )

    picked = pick_rows(spread.reshape(nta * rows, lines, LANES), rank)
    sent = lax.all_to_all(picked.reshape(nta, tl * lines, LANES), TA, 0, 0, tiled=True)
    sent = sent.reshape(nta * tl * lines, LANES)

    piece = 2 * per_x // near
    pair = pl.pallas_call(
        functools.partial(product_kernel, part, tl),
        out_shape=jax.ShapeDtypeStruct((near, nx, nsrc, tl, piece, ns * n), jnp.float32),
        in_specs=[vmem] * (1 + 2 * tl),
        out_specs=vmem,
        scratch_shapes=[pltpu.VMEM((tl, 4 * mine, wide), jnp.bfloat16)] * 2,
        compiler_params=small(12),
        name="product",
    )(sent, *cut)

    pair = pair.reshape(near * nx * nsrc, tl, piece, ns * n)
    got = lax.all_to_all(pair, ("tp", "xyz", "src"), 0, 0, tiled=True)
    back = pl.pallas_call(
        sum_kernel,
        out_shape=jax.ShapeDtypeStruct((nta * rows, nsrc, piece, ns * n), jnp.float32),
        in_specs=[smem, vmem],
        out_specs=vmem,
        scratch_shapes=[pltpu.VMEM((near * tl, nsrc, piece, ns * n), jnp.float32)],
        compiler_params=small(4),
        name="sum_over_xyz",
    )(here, got.reshape(near, nx, nsrc, tl, piece, ns * n))

    home = lax.all_to_all(back.reshape(nta, rows, nsrc, piece, ns * n), TA, 0, 0, tiled=True)
    home = home.reshape(nta // near, near, rows, nsrc, piece, ns * n)
    out = pl.pallas_call(
        functools.partial(final_kernel, near * tl),
        out_shape=jax.ShapeDtypeStruct((rows, 2, ns, nsrc * per_x, n), jnp.float32),
        in_specs=[
            pl.BlockSpec(memory_space=pltpu.SMEM),
            pl.BlockSpec(memory_space=pltpu.VMEM),
        ],
        out_specs=pl.BlockSpec(memory_space=pltpu.VMEM),
        compiler_params=small(4),
        name="final",
    )(wanted, home)
    return out.transpose(0, 1, 2, 4, 3)


def solution(mesh):
    shape = dict(mesh.shape)
    cut = (shape["job"], shape["ta"] // NEAR, NEAR, shape["xyz"], shape["src"])
    mesh = Mesh(mesh.devices.reshape(cut), ("job", *TA, "xyz", "src"))
    in_specs = (
        P("src", TA, None, "job", None, "xyz"),
        P(TA, "job", None, None, "xyz"),
        P(),
        P("src"),
    )
    out_specs = P(TA, None, "job", "src", "xyz")
    return jax.shard_map(local, mesh=mesh, in_specs=in_specs, out_specs=out_specs, check_vma=False)
```

```python
import functools

import jax
import jax.numpy as jnp
from jax import lax
from jax.experimental import pallas as pl
from jax.experimental.pallas import tpu as pltpu
from jax.sharding import Mesh
from jax.sharding import PartitionSpec as P


LANES = 128


def rank_of(keys):
    extent = keys.shape[0]
    index = jnp.arange(extent, dtype=jnp.int32)
    before = (keys[None, :] < keys[:, None]) | (
        (keys[None, :] == keys[:, None]) & (index[None, :] < index[:, None])
    )
    return jnp.sum(before.astype(jnp.int32), axis=1)


def inverse_of(rank):
    extent = rank.shape[0]
    index = jnp.arange(extent, dtype=jnp.int32)
    hit = rank[None, :] == index[:, None]
    return jnp.sum(jnp.where(hit, index[None, :], 0), axis=1)


def small(mib):
    return pltpu.CompilerParams(vmem_limit_bytes=mib << 20)


def share_kernel(core_ref, in_ref, out_ref, held, packed, sem, out_sem):
    rows, parts, folds, _, per_x, nc, _, sites = in_ref.shape
    core = core_ref[0]
    copies = [
        pltpu.make_async_copy(
            in_ref.at[r, i, :, core], held.at[r * parts + i], sem.at[r * parts + i]
        )
        for r in range(rows)
        for i in range(parts)
    ]
    for copy in copies:
        copy.start()
    lines = out_ref.shape[1] // rows
    sends = []
    for r in range(rows):
        line = r * lines
        for i in range(parts):
            p = r * parts + i
            copies[p].wait()
            for c in range(nc):
                for lane in range(0, sites, LANES):
                    for f in range(folds):
                        value = held[p, f, :, c, :, lane : lane + LANES]
                        packed[f * per_x : (f + 1) * per_x, line : line + 2, :] = value
                    line += 2
        span = pl.ds(r * lines, lines)
        sends.append(
            pltpu.make_async_copy(packed.at[:, span], out_ref.at[:, span], out_sem.at[r])
        )
        sends[-1].start()
    for send in sends:
        send.wait()


def pick_rows_kernel(index_ref, table_ref, out_ref):
    for i in range(out_ref.shape[0]):
        out_ref[i] = table_ref[index_ref[i]]


def pick_rows(table, index):
    count = index.shape[0]
    return pl.pallas_call(
        pick_rows_kernel,
        out_shape=jax.ShapeDtypeStruct((count, *table.shape[1:]), table.dtype),
        in_specs=[
            pl.BlockSpec(memory_space=pltpu.SMEM),
            pl.BlockSpec(memory_space=pltpu.VMEM),
        ],
        out_specs=pl.BlockSpec(memory_space=pltpu.VMEM),
        compiler_params=small(4),
        name="pick_rows",
    )(index, table)


def halves(x):
    high = x.astype(jnp.bfloat16)
    low = (x - high.astype(jnp.float32)).astype(jnp.bfloat16)
    return high, low


def split_kernel(core_ref, own_ref, other_ref, *outs):
    tl, _, width, _ = own_ref.shape
    core = core_ref[0]
    for slot, ref in ((core, own_ref), (1 - core, other_ref)):
        span = pl.ds(pl.multiple_of(slot * width, width), width)
        for t in range(tl):
            for ri in range(2):
                high, low = halves(ref[t, ri])
                outs[t][ri, span, :] = high
                outs[tl + t][ri, span, :] = low


def product_kernel(parts, tl, v_ref, *refs):
    p_hi, p_lo = refs[:tl], refs[tl : 2 * tl]
    out_ref, a_ref, b_ref = refs[2 * tl :]
    nq, nx, nsrc, _, piece, width = out_ref.shape
    cols = p_hi[0].shape[2] // LANES
    half = a_ref.shape[1] // 4
    nz = half // parts

    def dot(left, right):
        return lax.dot_general(
            left, right, (((1,), (1,)), ((), ())), preferred_element_type=jnp.float32
        )

    stride = tl * parts * cols * 2
    per = half // nx
    for t in range(tl):
        for i in range(parts):
            for b in range(cols):
                start = ((t * parts + i) * cols + b) * 2
                real_hi, real_lo = halves(v_ref[pl.ds(start, nz, stride=stride), :])
                imag_hi, imag_lo = halves(v_ref[pl.ds(start + 1, nz, stride=stride), :])
                lane = pl.ds(b * LANES, LANES)
                for j, (real, imag) in enumerate(((real_hi, imag_hi), (real_lo, imag_lo))):
                    top = pl.ds(2 * j * half + i * nz, nz)
                    low = pl.ds((2 * j + 1) * half + i * nz, nz)
                    a_ref[t, top, lane] = real
                    a_ref[t, low, lane] = -imag
                    b_ref[t, top, lane] = imag
                    b_ref[t, low, lane] = real
        both = dot(a_ref[t], p_hi[t][0]) + dot(b_ref[t], p_hi[t][1])
        total = both[: 2 * half] + both[2 * half :]
        total += dot(a_ref[t, : 2 * half], p_lo[t][0]) + dot(b_ref[t, : 2 * half], p_lo[t][1])
        for q in range(nq):
            ri, part = divmod(q, nq // 2)
            for x in range(nx):
                first = ri * half + x * per + part * piece
                for slot in range(nsrc):
                    out_ref[q, x, slot, t] = total[
                        first : first + piece, slot * width : (slot + 1) * width
                    ]


def sum_kernel(index_ref, in_ref, out_ref, held):
    near, nx, nsrc, tl = in_ref.shape[:4]
    nta, _, rows = out_ref.shape[:3]
    for z in range(near):
        total = in_ref[z, 0]
        for x in range(1, nx):
            total += in_ref[z, x]
        for t in range(tl):
            for core in range(nsrc):
                held[z * tl + t, core] = total[core, t]
    for ta in range(nta):
        for row in range(rows):
            value = held[index_ref[ta * rows + row]]
            for core in range(nsrc):
                out_ref[ta, core, row] = value[core]


def final_kernel(per_group, order_ref, in_ref, out_ref):
    _, nq, nsrc, rows, piece, _ = in_ref.shape
    ns, n = out_ref.shape[2], out_ref.shape[4]
    parts = nq // 2
    for row in range(rows):
        group = order_ref[row] // per_group
        for core in range(nsrc):
            for ri in range(2):
                for part in range(parts):
                    value = in_ref[group, ri * parts + part, core, row]
                    first = (core * parts + part) * piece
                    for s in range(ns):
                        out_ref[row, ri, s, first : first + piece, :] = value[
                            :, s * n : (s + 1) * n
                        ]


TA = ("tq", "tp")
NEAR = 4


def local(spinors, eigvecs, group_of, source_ids):
    nta, nx, nsrc = lax.axis_size(TA), lax.axis_size("xyz"), lax.axis_size("src")
    near = lax.axis_size("tp")
    core = lax.axis_index("src").astype(jnp.int32)
    ta = lax.axis_index(TA).astype(jnp.int32)
    rows, k, _, nc, sites = eigvecs.shape
    n, tl, _, ns = spinors.shape[:4]
    mine = k // nsrc
    part = mine // nta
    per_x = mine // nx
    fold = nta // per_x

    rank = rank_of(group_of)
    ordering = inverse_of(rank)

    tail = (nc, 2, sites)
    lines = part * nc * 2 * sites // LANES
    share = pl.pallas_call(
        share_kernel,
        out_shape=jax.ShapeDtypeStruct((nta, lines * rows, LANES), jnp.float32),
        in_specs=[
            pl.BlockSpec(memory_space=pltpu.SMEM),
            pl.BlockSpec(memory_space=pltpu.HBM),
        ],
        out_specs=pl.BlockSpec(memory_space=pltpu.HBM),
        scratch_shapes=[
            pltpu.VMEM((rows * part, fold, per_x, *tail), jnp.float32),
            pltpu.VMEM((nta, lines * rows, LANES), jnp.float32),
            pltpu.SemaphoreType.DMA((rows * part,)),
            pltpu.SemaphoreType.DMA((rows,)),
        ],
        name="share",
    )(
        core[None],
        eigvecs.transpose(0, 1, 3, 2, 4).reshape(rows, part, fold, nsrc, per_x, *tail),
    )
    spread = lax.all_to_all(share, TA, 0, 0, tiled=True)
    inverse = inverse_of(source_ids - n * core)
    held = spinors.at[inverse].get(mode="promise_in_bounds")
    held = held.transpose(1, 2, 3, 0, 4, 5).reshape(tl, 2, ns * n, nc * sites)
    other = lax.ppermute(held, "src", [(i, nsrc - 1 - i) for i in range(nsrc)])

    vmem = pl.BlockSpec(memory_space=pltpu.VMEM)
    smem = pl.BlockSpec(memory_space=pltpu.SMEM)
    wide = nc * sites
    cut = pl.pallas_call(
        split_kernel,
        out_shape=[pltpu.VMEM((2, nsrc * ns * n, wide), jnp.bfloat16)] * (2 * tl),
        in_specs=[smem, vmem, vmem],
        out_specs=[vmem] * (2 * tl),
        compiler_params=small(60),
        name="split",
    )(core[None], held, other)

    here = jnp.clip(ordering - (ta // near) * (near * tl), 0, near * tl - 1)
    wanted = lax.dynamic_slice_in_dim(ordering, ta * rows, rows, 0)
    spread, rank, here, wanted, *cut = lax.optimization_barrier(
        (spread, rank, here, wanted, *cut)
    )

    picked = pick_rows(spread.reshape(nta * rows, lines, LANES), rank)
    sent = lax.all_to_all(picked.reshape(nta, tl * lines, LANES), TA, 0, 0, tiled=True)
    sent = sent.reshape(nta * tl * lines, LANES)

    piece = 2 * per_x // near
    pair = pl.pallas_call(
        functools.partial(product_kernel, part, tl),
        out_shape=jax.ShapeDtypeStruct((near, nx, nsrc, tl, piece, ns * n), jnp.float32),
        in_specs=[vmem] * (1 + 2 * tl),
        out_specs=vmem,
        scratch_shapes=[pltpu.VMEM((tl, 4 * mine, wide), jnp.bfloat16)] * 2,
        compiler_params=small(12),
        name="product",
    )(sent, *cut)

    pair = pair.reshape(near * nx, nsrc, tl, piece, ns * n)
    got = lax.all_to_all(pair, ("tp", "xyz"), 0, 0, tiled=True)
    back = pl.pallas_call(
        sum_kernel,
        out_shape=jax.ShapeDtypeStruct((nta, nsrc, rows, piece, ns * n), jnp.float32),
        in_specs=[smem, vmem],
        out_specs=vmem,
        scratch_shapes=[pltpu.VMEM((near * tl, nsrc, piece, ns * n), jnp.float32)],
        compiler_params=small(4),
        name="sum_over_xyz",
    )(here, got.reshape(near, nx, nsrc, tl, piece, ns * n))

    back = back.reshape(nta * nsrc, rows, piece, ns * n)
    home = lax.all_to_all(back, (*TA, "src"), 0, 0, tiled=True)
    home = home.reshape(nta // near, near, nsrc, rows, piece, ns * n)
    out = pl.pallas_call(
        functools.partial(final_kernel, near * tl),
        out_shape=jax.ShapeDtypeStruct((rows, 2, ns, nsrc * per_x, n), jnp.float32),
        in_specs=[
            pl.BlockSpec(memory_space=pltpu.SMEM),
            pl.BlockSpec(memory_space=pltpu.VMEM),
        ],
        out_specs=pl.BlockSpec(memory_space=pltpu.VMEM),
        compiler_params=small(4),
        name="final",
    )(wanted, home)
    return out.transpose(0, 1, 2, 4, 3)


def solution(mesh):
    shape = dict(mesh.shape)
    cut = (shape["job"], shape["ta"] // NEAR, NEAR, shape["xyz"], shape["src"])
    mesh = Mesh(mesh.devices.reshape(cut), ("job", *TA, "xyz", "src"))
    in_specs = (
        P("src", TA, None, "job", None, "xyz"),
        P(TA, "job", None, None, "xyz"),
        P(),
        P("src"),
    )
    out_specs = P(TA, None, "job", "src", "xyz")
    return jax.shard_map(local, mesh=mesh, in_specs=in_specs, out_specs=out_specs, check_vma=False)
```

```python
import functools

import jax
import jax.numpy as jnp
from jax import lax
from jax.experimental import pallas as pl
from jax.experimental.pallas import tpu as pltpu
from jax.sharding import Mesh
from jax.sharding import PartitionSpec as P


LANES = 128


def rank_of(keys):
    extent = keys.shape[0]
    index = jnp.arange(extent, dtype=jnp.int32)
    before = (keys[None, :] < keys[:, None]) | (
        (keys[None, :] == keys[:, None]) & (index[None, :] < index[:, None])
    )
    return jnp.sum(before.astype(jnp.int32), axis=1)


def inverse_of(rank):
    extent = rank.shape[0]
    index = jnp.arange(extent, dtype=jnp.int32)
    hit = rank[None, :] == index[:, None]
    return jnp.sum(jnp.where(hit, index[None, :], 0), axis=1)


def small(mib):
    return pltpu.CompilerParams(vmem_limit_bytes=mib << 20)


def share_kernel(core_ref, in_ref, out_ref, held, packed, sem, out_sem):
    rows, parts, folds, _, per_x, nc, _, sites = in_ref.shape
    core = core_ref[0]
    copies = [
        pltpu.make_async_copy(
            in_ref.at[r, i, :, core], held.at[r * parts + i], sem.at[r * parts + i]
        )
        for r in range(rows)
        for i in range(parts)
    ]
    for copy in copies:
        copy.start()
    lines = out_ref.shape[1] // rows
    sends = []
    for r in range(rows):
        line = r * lines
        for i in range(parts):
            p = r * parts + i
            copies[p].wait()
            for c in range(nc):
                for lane in range(0, sites, LANES):
                    for f in range(folds):
                        value = held[p, f, :, c, :, lane : lane + LANES]
                        packed[f * per_x : (f + 1) * per_x, line : line + 2, :] = value
                    line += 2
        span = pl.ds(r * lines, lines)
        sends.append(
            pltpu.make_async_copy(packed.at[:, span], out_ref.at[:, span], out_sem.at[r])
        )
        sends[-1].start()
    for send in sends:
        send.wait()


def pick_rows_kernel(index_ref, table_ref, out_ref):
    for i in range(out_ref.shape[0]):
        out_ref[i] = table_ref[index_ref[i]]


def pick_rows(table, index):
    count = index.shape[0]
    return pl.pallas_call(
        pick_rows_kernel,
        out_shape=jax.ShapeDtypeStruct((count, *table.shape[1:]), table.dtype),
        in_specs=[
            pl.BlockSpec(memory_space=pltpu.SMEM),
            pl.BlockSpec(memory_space=pltpu.VMEM),
        ],
        out_specs=pl.BlockSpec(memory_space=pltpu.VMEM),
        compiler_params=small(4),
        name="pick_rows",
    )(index, table)


def halves(x):
    high = x.astype(jnp.bfloat16)
    low = (x - high.astype(jnp.float32)).astype(jnp.bfloat16)
    return high, low


def split_kernel(core_ref, own_ref, other_ref, *outs):
    tl, _, width, _ = own_ref.shape
    core = core_ref[0]
    for slot, ref in ((core, own_ref), (1 - core, other_ref)):
        span = pl.ds(pl.multiple_of(slot * width, width), width)
        for t in range(tl):
            for ri in range(2):
                high, low = halves(ref[t, ri])
                outs[t][ri, span, :] = high
                outs[tl + t][ri, span, :] = low


def product_kernel(parts, tl, v_ref, *refs):
    p_hi, p_lo = refs[:tl], refs[tl : 2 * tl]
    out_ref, a_ref, b_ref = refs[2 * tl :]
    nq, nx, nsrc, _, piece, width = out_ref.shape
    cols = p_hi[0].shape[2] // LANES
    half = a_ref.shape[1] // 4
    nz = half // parts

    def dot(left, right):
        return lax.dot_general(
            left, right, (((1,), (1,)), ((), ())), preferred_element_type=jnp.float32
        )

    stride = tl * parts * cols * 2
    per = half // nx
    for t in range(tl):
        for i in range(parts):
            for b in range(cols):
                start = ((t * parts + i) * cols + b) * 2
                real_hi, real_lo = halves(v_ref[pl.ds(start, nz, stride=stride), :])
                imag_hi, imag_lo = halves(v_ref[pl.ds(start + 1, nz, stride=stride), :])
                lane = pl.ds(b * LANES, LANES)
                for j, (real, imag) in enumerate(((real_hi, imag_hi), (real_lo, imag_lo))):
                    top = pl.ds(2 * j * half + i * nz, nz)
                    low = pl.ds((2 * j + 1) * half + i * nz, nz)
                    a_ref[t, top, lane] = real
                    a_ref[t, low, lane] = -imag
                    b_ref[t, top, lane] = imag
                    b_ref[t, low, lane] = real
        both = dot(a_ref[t], p_hi[t][0]) + dot(b_ref[t], p_hi[t][1])
        total = both[: 2 * half] + both[2 * half :]
        total += dot(a_ref[t, : 2 * half], p_lo[t][0]) + dot(b_ref[t, : 2 * half], p_lo[t][1])
        for q in range(nq):
            ri, part = divmod(q, nq // 2)
            for x in range(nx):
                first = ri * half + x * per + part * piece
                for slot in range(nsrc):
                    out_ref[q, x, slot, t] = total[
                        first : first + piece, slot * width : (slot + 1) * width
                    ]


def sum_kernel(index_ref, in_ref, out_ref, held):
    near, nx, nsrc, tl = in_ref.shape[:4]
    for z in range(near):
        total = in_ref[z, 0]
        for x in range(1, nx):
            total += in_ref[z, x]
        for t in range(tl):
            for core in range(nsrc):
                held[z * tl + t, core] = total[core, t]
    for row in range(out_ref.shape[0]):
        out_ref[row] = held[index_ref[row]]


def final_kernel(per_group, order_ref, in_ref, out_ref):
    _, nq, rows, nsrc, piece, _ = in_ref.shape
    ns, n = out_ref.shape[2], out_ref.shape[4]
    parts = nq // 2
    for row in range(rows):
        group = order_ref[row] // per_group
        for core in range(nsrc):
            for ri in range(2):
                for part in range(parts):
                    value = in_ref[group, ri * parts + part, row, core]
                    first = (core * parts + part) * piece
                    for s in range(ns):
                        out_ref[row, ri, s, first : first + piece, :] = value[
                            :, s * n : (s + 1) * n
                        ]


TA = ("tq", "tp")
NEAR = 4


def local(spinors, eigvecs, group_of, source_ids):
    nta, nx, nsrc = lax.axis_size(TA), lax.axis_size("xyz"), lax.axis_size("src")
    near = lax.axis_size("tp")
    core = lax.axis_index("src").astype(jnp.int32)
    ta = lax.axis_index(TA).astype(jnp.int32)
    rows, k, _, nc, sites = eigvecs.shape
    n, tl, _, ns = spinors.shape[:4]
    mine = k // nsrc
    part = mine // nta
    per_x = mine // nx
    fold = nta // per_x

    rank = rank_of(group_of)

    tail = (nc, 2, sites)
    lines = part * nc * 2 * sites // LANES
    share = pl.pallas_call(
        share_kernel,
        out_shape=jax.ShapeDtypeStruct((nta, lines * rows, LANES), jnp.float32),
        in_specs=[
            pl.BlockSpec(memory_space=pltpu.SMEM),
            pl.BlockSpec(memory_space=pltpu.HBM),
        ],
        out_specs=pl.BlockSpec(memory_space=pltpu.HBM),
        scratch_shapes=[
            pltpu.VMEM((rows * part, fold, per_x, *tail), jnp.float32),
            pltpu.VMEM((nta, lines * rows, LANES), jnp.float32),
            pltpu.SemaphoreType.DMA((rows * part,)),
            pltpu.SemaphoreType.DMA((rows,)),
        ],
        name="share",
    )(
        core[None],
        eigvecs.transpose(0, 1, 3, 2, 4).reshape(rows, part, fold, nsrc, per_x, *tail),
    )
    spread = lax.all_to_all(share, TA, 0, 0, tiled=True)
    inverse = inverse_of(source_ids - n * core)
    held = spinors.at[inverse].get(mode="promise_in_bounds")
    held = held.transpose(1, 2, 3, 0, 4, 5).reshape(tl, 2, ns * n, nc * sites)
    other = lax.ppermute(held, "src", [(i, nsrc - 1 - i) for i in range(nsrc)])

    vmem = pl.BlockSpec(memory_space=pltpu.VMEM)
    smem = pl.BlockSpec(memory_space=pltpu.SMEM)
    wide = nc * sites
    cut = pl.pallas_call(
        split_kernel,
        out_shape=[pltpu.VMEM((2, nsrc * ns * n, wide), jnp.bfloat16)] * (2 * tl),
        in_specs=[smem, vmem, vmem],
        out_specs=[vmem] * (2 * tl),
        compiler_params=small(60),
        name="split",
    )(core[None], held, other)

    spread, rank, *cut = lax.optimization_barrier((spread, rank, *cut))

    picked = pick_rows(spread.reshape(nta * rows, lines, LANES), rank)
    sent = lax.all_to_all(picked.reshape(nta, tl * lines, LANES), TA, 0, 0, tiled=True)
    sent = sent.reshape(nta * tl * lines, LANES)

    order = inverse_of(rank)
    here = jnp.clip(order - (ta // near) * (near * tl), 0, near * tl - 1)
    wanted = lax.dynamic_slice_in_dim(order, ta * rows, rows, 0)
    sent, here, wanted = lax.optimization_barrier((sent, here, wanted))

    piece = 2 * per_x // near
    pair = pl.pallas_call(
        functools.partial(product_kernel, part, tl),
        out_shape=jax.ShapeDtypeStruct((near, nx, nsrc, tl, piece, ns * n), jnp.float32),
        in_specs=[vmem] * (1 + 2 * tl),
        out_specs=vmem,
        scratch_shapes=[pltpu.VMEM((tl, 4 * mine, wide), jnp.bfloat16)] * 2,
        compiler_params=small(12),
        name="product",
    )(sent, *cut)

    pair = pair.reshape(near * nx * nsrc, tl, piece, ns * n)
    got = lax.all_to_all(pair, ("tp", "xyz", "src"), 0, 0, tiled=True)
    back = pl.pallas_call(
        sum_kernel,
        out_shape=jax.ShapeDtypeStruct((nta * rows, nsrc, piece, ns * n), jnp.float32),
        in_specs=[smem, vmem],
        out_specs=vmem,
        scratch_shapes=[pltpu.VMEM((near * tl, nsrc, piece, ns * n), jnp.float32)],
        compiler_params=small(4),
        name="sum_over_xyz",
    )(here, got.reshape(near, nx, nsrc, tl, piece, ns * n))

    home = lax.all_to_all(back.reshape(nta, rows, nsrc, piece, ns * n), TA, 0, 0, tiled=True)
    home = home.reshape(nta // near, near, rows, nsrc, piece, ns * n)
    out = pl.pallas_call(
        functools.partial(final_kernel, near * tl),
        out_shape=jax.ShapeDtypeStruct((rows, 2, ns, nsrc * per_x, n), jnp.float32),
        in_specs=[
            pl.BlockSpec(memory_space=pltpu.SMEM),
            pl.BlockSpec(memory_space=pltpu.VMEM),
        ],
        out_specs=pl.BlockSpec(memory_space=pltpu.VMEM),
        compiler_params=small(4),
        name="final",
    )(wanted, home)
    return out.transpose(0, 1, 2, 4, 3)


def solution(mesh):
    shape = dict(mesh.shape)
    cut = (shape["job"], shape["ta"] // NEAR, NEAR, shape["xyz"], shape["src"])
    mesh = Mesh(mesh.devices.reshape(cut), ("job", *TA, "xyz", "src"))
    in_specs = (
        P("src", TA, None, "job", None, "xyz"),
        P(TA, "job", None, None, "xyz"),
        P(),
        P("src"),
    )
    out_specs = P(TA, None, "job", "src", "xyz")
    return jax.shard_map(local, mesh=mesh, in_specs=in_specs, out_specs=out_specs, check_vma=False)
```

```python
import functools

import jax
import jax.numpy as jnp
from jax import lax
from jax.experimental import pallas as pl
from jax.experimental.pallas import tpu as pltpu
from jax.sharding import Mesh
from jax.sharding import PartitionSpec as P


LANES = 128


def rank_of(keys):
    extent = keys.shape[0]
    index = jnp.arange(extent, dtype=jnp.int32)
    before = (keys[None, :] < keys[:, None]) | (
        (keys[None, :] == keys[:, None]) & (index[None, :] < index[:, None])
    )
    return jnp.sum(before.astype(jnp.int32), axis=1)


def inverse_of(rank):
    extent = rank.shape[0]
    index = jnp.arange(extent, dtype=jnp.int32)
    hit = rank[None, :] == index[:, None]
    return jnp.sum(jnp.where(hit, index[None, :], 0), axis=1)


def small(mib):
    return pltpu.CompilerParams(vmem_limit_bytes=mib << 20)


def share_kernel(core_ref, in_ref, out_ref, held, packed, sem, out_sem):
    rows, parts, folds, _, per_x, nc, _, sites = in_ref.shape
    core = core_ref[0]
    copies = [
        pltpu.make_async_copy(
            in_ref.at[r, i, :, core], held.at[r * parts + i], sem.at[r * parts + i]
        )
        for r in range(rows)
        for i in range(parts)
    ]
    for copy in copies:
        copy.start()
    lines = out_ref.shape[1] // rows
    sends = []
    for r in range(rows):
        line = r * lines
        for i in range(parts):
            p = r * parts + i
            copies[p].wait()
            for c in range(nc):
                for lane in range(0, sites, LANES):
                    for f in range(folds):
                        value = held[p, f, :, c, :, lane : lane + LANES]
                        packed[f * per_x : (f + 1) * per_x, line : line + 2, :] = value
                    line += 2
        span = pl.ds(r * lines, lines)
        sends.append(
            pltpu.make_async_copy(packed.at[:, span], out_ref.at[:, span], out_sem.at[r])
        )
        sends[-1].start()
    for send in sends:
        send.wait()


def pick_rows_kernel(index_ref, table_ref, out_ref):
    for i in range(out_ref.shape[0]):
        out_ref[i] = table_ref[index_ref[i]]


def pick_rows(table, index):
    count = index.shape[0]
    return pl.pallas_call(
        pick_rows_kernel,
        out_shape=jax.ShapeDtypeStruct((count, *table.shape[1:]), table.dtype),
        in_specs=[
            pl.BlockSpec(memory_space=pltpu.SMEM),
            pl.BlockSpec(memory_space=pltpu.VMEM),
        ],
        out_specs=pl.BlockSpec(memory_space=pltpu.VMEM),
        compiler_params=small(4),
        name="pick_rows",
    )(index, table)


def halves(x):
    high = x.astype(jnp.bfloat16)
    low = (x - high.astype(jnp.float32)).astype(jnp.bfloat16)
    return high, low


def split_kernel(core_ref, own_ref, other_ref, *outs):
    tl, _, width, _ = own_ref.shape
    core = core_ref[0]
    for slot, ref in ((core, own_ref), (1 - core, other_ref)):
        span = pl.ds(pl.multiple_of(slot * width, width), width)
        for t in range(tl):
            for ri in range(2):
                high, low = halves(ref[t, ri])
                outs[t][ri, span, :] = high
                outs[tl + t][ri, span, :] = low


def product_kernel(parts, tl, v_ref, *refs):
    p_hi, p_lo = refs[:tl], refs[tl : 2 * tl]
    out_ref, a_ref, b_ref = refs[2 * tl :]
    nx, nq, nsrc, _, piece, width = out_ref.shape
    cols = p_hi[0].shape[2] // LANES
    half = a_ref.shape[1] // 4
    nz = half // parts

    def dot(left, right):
        return lax.dot_general(
            left, right, (((1,), (1,)), ((), ())), preferred_element_type=jnp.float32
        )

    stride = tl * parts * cols * 2
    per = half // nx
    for t in range(tl):
        for i in range(parts):
            for b in range(cols):
                start = ((t * parts + i) * cols + b) * 2
                real_hi, real_lo = halves(v_ref[pl.ds(start, nz, stride=stride), :])
                imag_hi, imag_lo = halves(v_ref[pl.ds(start + 1, nz, stride=stride), :])
                lane = pl.ds(b * LANES, LANES)
                for j, (real, imag) in enumerate(((real_hi, imag_hi), (real_lo, imag_lo))):
                    top = pl.ds(2 * j * half + i * nz, nz)
                    low = pl.ds((2 * j + 1) * half + i * nz, nz)
                    a_ref[t, top, lane] = real
                    a_ref[t, low, lane] = -imag
                    b_ref[t, top, lane] = imag
                    b_ref[t, low, lane] = real
        both = dot(a_ref[t], p_hi[t][0]) + dot(b_ref[t], p_hi[t][1])
        total = both[: 2 * half] + both[2 * half :]
        total += dot(a_ref[t, : 2 * half], p_lo[t][0]) + dot(b_ref[t, : 2 * half], p_lo[t][1])
        for q in range(nq):
            ri, part = divmod(q, nq // 2)
            for x in range(nx):
                first = ri * half + x * per + part * piece
                for slot in range(nsrc):
                    out_ref[x, q, slot, t] = total[
                        first : first + piece, slot * width : (slot + 1) * width
                    ]


def sum_kernel(index_ref, in_ref, out_ref, held):
    nx, near, nsrc, tl = in_ref.shape[:4]
    for z in range(near):
        total = in_ref[0, z]
        for x in range(1, nx):
            total += in_ref[x, z]
        for t in range(tl):
            for core in range(nsrc):
                held[z * tl + t, core] = total[core, t]
    for row in range(out_ref.shape[0]):
        out_ref[row] = held[index_ref[row]]


def final_kernel(per_group, order_ref, in_ref, out_ref):
    _, nq, rows, nsrc, piece, _ = in_ref.shape
    ns, n = out_ref.shape[2], out_ref.shape[4]
    parts = nq // 2
    for row in range(rows):
        group = order_ref[row] // per_group
        for core in range(nsrc):
            for ri in range(2):
                for part in range(parts):
                    value = in_ref[group, ri * parts + part, row, core]
                    first = (core * parts + part) * piece
                    for s in range(ns):
                        out_ref[row, ri, s, first : first + piece, :] = value[
                            :, s * n : (s + 1) * n
                        ]


TA = ("tq", "tp")
NEAR = 4


def local(spinors, eigvecs, group_of, source_ids):
    nta, nx, nsrc = lax.axis_size(TA), lax.axis_size("xyz"), lax.axis_size("src")
    near = lax.axis_size("tp")
    core = lax.axis_index("src").astype(jnp.int32)
    ta = lax.axis_index(TA).astype(jnp.int32)
    rows, k, _, nc, sites = eigvecs.shape
    n, tl, _, ns = spinors.shape[:4]
    mine = k // nsrc
    part = mine // nta
    per_x = mine // nx
    fold = nta // per_x

    rank = rank_of(group_of)
    ordering = inverse_of(rank)

    tail = (nc, 2, sites)
    lines = part * nc * 2 * sites // LANES
    share = pl.pallas_call(
        share_kernel,
        out_shape=jax.ShapeDtypeStruct((nta, lines * rows, LANES), jnp.float32),
        in_specs=[
            pl.BlockSpec(memory_space=pltpu.SMEM),
            pl.BlockSpec(memory_space=pltpu.HBM),
        ],
        out_specs=pl.BlockSpec(memory_space=pltpu.HBM),
        scratch_shapes=[
            pltpu.VMEM((rows * part, fold, per_x, *tail), jnp.float32),
            pltpu.VMEM((nta, lines * rows, LANES), jnp.float32),
            pltpu.SemaphoreType.DMA((rows * part,)),
            pltpu.SemaphoreType.DMA((rows,)),
        ],
        name="share",
    )(
        core[None],
        eigvecs.transpose(0, 1, 3, 2, 4).reshape(rows, part, fold, nsrc, per_x, *tail),
    )
    spread = lax.all_to_all(share, TA, 0, 0, tiled=True)
    inverse = inverse_of(source_ids - n * core)
    held = spinors.at[inverse].get(mode="promise_in_bounds")
    held = held.transpose(1, 2, 3, 0, 4, 5).reshape(tl, 2, ns * n, nc * sites)
    other = lax.ppermute(held, "src", [(i, nsrc - 1 - i) for i in range(nsrc)])

    vmem = pl.BlockSpec(memory_space=pltpu.VMEM)
    smem = pl.BlockSpec(memory_space=pltpu.SMEM)
    wide = nc * sites
    cut = pl.pallas_call(
        split_kernel,
        out_shape=[pltpu.VMEM((2, nsrc * ns * n, wide), jnp.bfloat16)] * (2 * tl),
        in_specs=[smem, vmem, vmem],
        out_specs=[vmem] * (2 * tl),
        compiler_params=small(60),
        name="split",
    )(core[None], held, other)

    here = jnp.clip(ordering - (ta // near) * (near * tl), 0, near * tl - 1)
    wanted = lax.dynamic_slice_in_dim(ordering, ta * rows, rows, 0)
    spread, rank, here, wanted, *cut = lax.optimization_barrier(
        (spread, rank, here, wanted, *cut)
    )

    picked = pick_rows(spread.reshape(nta * rows, lines, LANES), rank)
    sent = lax.all_to_all(picked.reshape(nta, tl * lines, LANES), TA, 0, 0, tiled=True)
    sent = sent.reshape(nta * tl * lines, LANES)

    piece = 2 * per_x // near
    pair = pl.pallas_call(
        functools.partial(product_kernel, part, tl),
        out_shape=jax.ShapeDtypeStruct((nx, near, nsrc, tl, piece, ns * n), jnp.float32),
        in_specs=[vmem] * (1 + 2 * tl),
        out_specs=vmem,
        scratch_shapes=[pltpu.VMEM((tl, 4 * mine, wide), jnp.bfloat16)] * 2,
        compiler_params=small(12),
        name="product",
    )(sent, *cut)

    pair = pair.reshape(nx * near * nsrc, tl, piece, ns * n)
    got = lax.all_to_all(pair, ("xyz", "tp", "src"), 0, 0, tiled=True)
    back = pl.pallas_call(
        sum_kernel,
        out_shape=jax.ShapeDtypeStruct((nta * rows, nsrc, piece, ns * n), jnp.float32),
        in_specs=[smem, vmem],
        out_specs=vmem,
        scratch_shapes=[pltpu.VMEM((near * tl, nsrc, piece, ns * n), jnp.float32)],
        compiler_params=small(4),
        name="sum_over_xyz",
    )(here, got.reshape(nx, near, nsrc, tl, piece, ns * n))

    home = lax.all_to_all(back.reshape(nta, rows, nsrc, piece, ns * n), TA, 0, 0, tiled=True)
    home = home.reshape(nta // near, near, rows, nsrc, piece, ns * n)
    out = pl.pallas_call(
        functools.partial(final_kernel, near * tl),
        out_shape=jax.ShapeDtypeStruct((rows, 2, ns, nsrc * per_x, n), jnp.float32),
        in_specs=[
            pl.BlockSpec(memory_space=pltpu.SMEM),
            pl.BlockSpec(memory_space=pltpu.VMEM),
        ],
        out_specs=pl.BlockSpec(memory_space=pltpu.VMEM),
        compiler_params=small(4),
        name="final",
    )(wanted, home)
    return out.transpose(0, 1, 2, 4, 3)


def solution(mesh):
    shape = dict(mesh.shape)
    cut = (shape["job"], shape["ta"] // NEAR, NEAR, shape["xyz"], shape["src"])
    mesh = Mesh(mesh.devices.reshape(cut), ("job", *TA, "xyz", "src"))
    in_specs = (
        P("src", TA, None, "job", None, "xyz"),
        P(TA, "job", None, None, "xyz"),
        P(),
        P("src"),
    )
    out_specs = P(TA, None, "job", "src", "xyz")
    return jax.shard_map(local, mesh=mesh, in_specs=in_specs, out_specs=out_specs, check_vma=False)
```

```python
import functools

import jax
import jax.numpy as jnp
from jax import lax
from jax.experimental import pallas as pl
from jax.experimental.pallas import tpu as pltpu
from jax.sharding import Mesh
from jax.sharding import PartitionSpec as P


LANES = 128


def rank_of(keys):
    extent = keys.shape[0]
    index = jnp.arange(extent, dtype=jnp.int32)
    before = (keys[None, :] < keys[:, None]) | (
        (keys[None, :] == keys[:, None]) & (index[None, :] < index[:, None])
    )
    return jnp.sum(before.astype(jnp.int32), axis=1)


def inverse_of(rank):
    extent = rank.shape[0]
    index = jnp.arange(extent, dtype=jnp.int32)
    hit = rank[None, :] == index[:, None]
    return jnp.sum(jnp.where(hit, index[None, :], 0), axis=1)


def small(mib):
    return pltpu.CompilerParams(vmem_limit_bytes=mib << 20)


def share_kernel(core_ref, in_ref, out_ref, held, packed, sem, out_sem):
    rows, parts, folds, _, per_x, nc, _, sites = in_ref.shape
    core = core_ref[0]
    copies = [
        pltpu.make_async_copy(
            in_ref.at[r, i, :, core], held.at[r * parts + i], sem.at[r * parts + i]
        )
        for r in range(rows)
        for i in range(parts)
    ]
    for copy in copies:
        copy.start()
    sends = []
    line = sent = 0
    for p, copy in enumerate(copies):
        copy.wait()
        for c in range(nc):
            for lane in range(0, sites, LANES):
                for f in range(folds):
                    value = held[p, f, :, c, :, lane : lane + LANES]
                    packed[f * per_x : (f + 1) * per_x, line : line + 2, :] = value
                line += 2
        if line % 8 == 0:
            span = pl.ds(sent, line - sent)
            sends.append(
                pltpu.make_async_copy(packed.at[:, span], out_ref.at[:, span], out_sem.at[p])
            )
            sends[-1].start()
            sent = line
    for send in sends:
        send.wait()


def pick_rows_kernel(index_ref, table_ref, out_ref):
    for i in range(out_ref.shape[0]):
        out_ref[i] = table_ref[index_ref[i]]


def pick_rows(table, index):
    count = index.shape[0]
    return pl.pallas_call(
        pick_rows_kernel,
        out_shape=jax.ShapeDtypeStruct((count, *table.shape[1:]), table.dtype),
        in_specs=[
            pl.BlockSpec(memory_space=pltpu.SMEM),
            pl.BlockSpec(memory_space=pltpu.VMEM),
        ],
        out_specs=pl.BlockSpec(memory_space=pltpu.VMEM),
        compiler_params=small(4),
        name="pick_rows",
    )(index, table)


def halves(x):
    high = x.astype(jnp.bfloat16)
    low = (x - high.astype(jnp.float32)).astype(jnp.bfloat16)
    return high, low


def split_kernel(core_ref, own_ref, other_ref, *outs):
    tl, _, width, _ = own_ref.shape
    core = core_ref[0]
    for slot, ref in ((core, own_ref), (1 - core, other_ref)):
        span = pl.ds(pl.multiple_of(slot * width, width), width)
        for t in range(tl):
            for ri in range(2):
                high, low = halves(ref[t, ri])
                outs[t][ri, span, :] = high
                outs[tl + t][ri, span, :] = low


def product_kernel(parts, tl, v_ref, *refs):
    p_hi, p_lo = refs[:tl], refs[tl : 2 * tl]
    out_ref, a_ref, b_ref = refs[2 * tl :]
    nq, nx, nsrc, _, piece, width = out_ref.shape
    cols = p_hi[0].shape[2] // LANES
    half = a_ref.shape[1] // 4
    nz = half // parts

    def dot(left, right):
        return lax.dot_general(
            left, right, (((1,), (1,)), ((), ())), preferred_element_type=jnp.float32
        )

    stride = tl * parts * cols * 2
    per = half // nx
    for t in range(tl):
        for i in range(parts):
            for b in range(cols):
                start = ((t * parts + i) * cols + b) * 2
                real_hi, real_lo = halves(v_ref[pl.ds(start, nz, stride=stride), :])
                imag_hi, imag_lo = halves(v_ref[pl.ds(start + 1, nz, stride=stride), :])
                lane = pl.ds(b * LANES, LANES)
                for j, (real, imag) in enumerate(((real_hi, imag_hi), (real_lo, imag_lo))):
                    top = pl.ds(2 * j * half + i * nz, nz)
                    low = pl.ds((2 * j + 1) * half + i * nz, nz)
                    a_ref[t, top, lane] = real
                    a_ref[t, low, lane] = -imag
                    b_ref[t, top, lane] = imag
                    b_ref[t, low, lane] = real
        both = dot(a_ref[t], p_hi[t][0]) + dot(b_ref[t], p_hi[t][1])
        total = both[: 2 * half] + both[2 * half :]
        total += dot(a_ref[t, : 2 * half], p_lo[t][0]) + dot(b_ref[t, : 2 * half], p_lo[t][1])
        for q in range(nq):
            ri, part = divmod(q, nq // 2)
            for x in range(nx):
                first = ri * half + x * per + part * piece
                for slot in range(nsrc):
                    out_ref[q, x, slot, t] = total[
                        first : first + piece, slot * width : (slot + 1) * width
                    ]


def sum_kernel(index_ref, in_ref, out_ref, held):
    near, nx, nsrc, tl = in_ref.shape[:4]
    for z in range(near):
        total = in_ref[z, 0]
        for x in range(1, nx):
            total += in_ref[z, x]
        for t in range(tl):
            for core in range(nsrc):
                held[z * tl + t, core] = total[core, t]
    for row in range(out_ref.shape[0]):
        out_ref[row] = held[index_ref[row]]


def final_kernel(per_group, order_ref, in_ref, out_ref):
    _, nq, rows, nsrc, piece, _ = in_ref.shape
    ns, n = out_ref.shape[2], out_ref.shape[4]
    parts = nq // 2
    for row in range(rows):
        group = order_ref[row] // per_group
        for core in range(nsrc):
            for ri in range(2):
                for part in range(parts):
                    value = in_ref[group, ri * parts + part, row, core]
                    first = (core * parts + part) * piece
                    for s in range(ns):
                        out_ref[row, ri, s, first : first + piece, :] = value[
                            :, s * n : (s + 1) * n
                        ]


TA = ("tq", "tp")
NEAR = 4


def local(spinors, eigvecs, group_of, source_ids):
    nta, nx, nsrc = lax.axis_size(TA), lax.axis_size("xyz"), lax.axis_size("src")
    near = lax.axis_size("tp")
    core = lax.axis_index("src").astype(jnp.int32)
    ta = lax.axis_index(TA).astype(jnp.int32)
    rows, k, _, nc, sites = eigvecs.shape
    n, tl, _, ns = spinors.shape[:4]
    mine = k // nsrc
    part = mine // nta
    per_x = mine // nx
    fold = nta // per_x

    rank = rank_of(group_of)
    ordering = inverse_of(rank)

    tail = (nc, 2, sites)
    lines = part * nc * 2 * sites // LANES
    share = pl.pallas_call(
        share_kernel,
        out_shape=jax.ShapeDtypeStruct((nta, lines * rows, LANES), jnp.float32),
        in_specs=[
            pl.BlockSpec(memory_space=pltpu.SMEM),
            pl.BlockSpec(memory_space=pltpu.HBM),
        ],
        out_specs=pl.BlockSpec(memory_space=pltpu.HBM),
        scratch_shapes=[
            pltpu.VMEM((rows * part, fold, per_x, *tail), jnp.float32),
            pltpu.VMEM((nta, lines * rows, LANES), jnp.float32),
            pltpu.SemaphoreType.DMA((rows * part,)),
            pltpu.SemaphoreType.DMA((rows * part,)),
        ],
        name="share",
    )(
        core[None],
        eigvecs.transpose(0, 1, 3, 2, 4).reshape(rows, part, fold, nsrc, per_x, *tail),
    )
    spread = lax.all_to_all(share, TA, 0, 0, tiled=True)
    inverse = inverse_of(source_ids - n * core)
    held = spinors.at[inverse].get(mode="promise_in_bounds")
    held = held.transpose(1, 2, 3, 0, 4, 5).reshape(tl, 2, ns * n, nc * sites)
    other = lax.ppermute(held, "src", [(i, nsrc - 1 - i) for i in range(nsrc)])

    vmem = pl.BlockSpec(memory_space=pltpu.VMEM)
    smem = pl.BlockSpec(memory_space=pltpu.SMEM)
    wide = nc * sites
    cut = pl.pallas_call(
        split_kernel,
        out_shape=[pltpu.VMEM((2, nsrc * ns * n, wide), jnp.bfloat16)] * (2 * tl),
        in_specs=[smem, vmem, vmem],
        out_specs=[vmem] * (2 * tl),
        compiler_params=small(60),
        name="split",
    )(core[None], held, other)

    here = jnp.clip(ordering - (ta // near) * (near * tl), 0, near * tl - 1)
    wanted = lax.dynamic_slice_in_dim(ordering, ta * rows, rows, 0)
    spread, rank, here, wanted, *cut = lax.optimization_barrier(
        (spread, rank, here, wanted, *cut)
    )

    picked = pick_rows(spread.reshape(nta * rows, lines, LANES), rank)
    sent = lax.all_to_all(picked.reshape(nta, tl * lines, LANES), TA, 0, 0, tiled=True)
    sent = sent.reshape(nta * tl * lines, LANES)

    piece = 2 * per_x // near
    pair = pl.pallas_call(
        functools.partial(product_kernel, part, tl),
        out_shape=jax.ShapeDtypeStruct((near, nx, nsrc, tl, piece, ns * n), jnp.float32),
        in_specs=[vmem] * (1 + 2 * tl),
        out_specs=vmem,
        scratch_shapes=[pltpu.VMEM((tl, 4 * mine, wide), jnp.bfloat16)] * 2,
        compiler_params=small(12),
        name="product",
    )(sent, *cut)

    pair = pair.reshape(near * nx * nsrc, tl, piece, ns * n)
    got = lax.all_to_all(pair, ("tp", "xyz", "src"), 0, 0, tiled=True)
    back = pl.pallas_call(
        sum_kernel,
        out_shape=jax.ShapeDtypeStruct((nta * rows, nsrc, piece, ns * n), jnp.float32),
        in_specs=[smem, vmem],
        out_specs=vmem,
        scratch_shapes=[pltpu.VMEM((near * tl, nsrc, piece, ns * n), jnp.float32)],
        compiler_params=small(4),
        name="sum_over_xyz",
    )(here, got.reshape(near, nx, nsrc, tl, piece, ns * n))

    home = lax.all_to_all(back.reshape(nta, rows, nsrc, piece, ns * n), TA, 0, 0, tiled=True)
    home = home.reshape(nta // near, near, rows, nsrc, piece, ns * n)
    out = pl.pallas_call(
        functools.partial(final_kernel, near * tl),
        out_shape=jax.ShapeDtypeStruct((rows, 2, ns, nsrc * per_x, n), jnp.float32),
        in_specs=[
            pl.BlockSpec(memory_space=pltpu.SMEM),
            pl.BlockSpec(memory_space=pltpu.VMEM),
        ],
        out_specs=pl.BlockSpec(memory_space=pltpu.VMEM),
        compiler_params=small(4),
        name="final",
    )(wanted, home)
    return out.transpose(0, 1, 2, 4, 3)


def solution(mesh):
    shape = dict(mesh.shape)
    cut = (shape["job"], shape["ta"] // NEAR, NEAR, shape["xyz"], shape["src"])
    mesh = Mesh(mesh.devices.reshape(cut), ("job", *TA, "xyz", "src"))
    in_specs = (
        P("src", TA, None, "job", None, "xyz"),
        P(TA, "job", None, None, "xyz"),
        P(),
        P("src"),
    )
    out_specs = P(TA, None, "job", "src", "xyz")
    return jax.shard_map(local, mesh=mesh, in_specs=in_specs, out_specs=out_specs, check_vma=False)
```
